16 devices in a mesh: dp: 2 (over y, z), tp: 8 (over x, core).
Axes of the slice: x: 4, y: 2, z: 1, core: 2. Of those that a mesh axis runs over, the one named last changes fastest.
The devices are a block of a 4x4x8 slice.
Arguments:
- token_ids: int32 [2, 1024], P('dp'), parts along dimension 0
- emb_table: bfloat16 [32000, 2048], P('tp')
- norm_gain: bfloat16 [2048], replicated
- grad_out: bfloat16 [2, 1024, 2048], P('dp', 'tp'), parts along dimension 0
Outputs:
- output 1: bfloat16 [2, 1024, 2048], P('dp', 'tp'), parts along dimension 0
- output 2: float32 [64000, 2048], P(('dp', 'tp')), parts along dimension 0
- output 3: float32 [4096], P('dp'), parts along dimension 0
There are 2 independent parts. The reference program is written for one: setup_inputs(seed, part) draws one part's arguments, and reference() takes and returns one part's arrays. A program takes and returns all parts, laid end to end along the dimension named above; an argument that names none is the same for every part.
All inputs are finite; a program needn't handle non-finite values.
Results may differ from the reference program's by a relative error of at most 0.0085353.
Values are sent between devices in bfloat16 or wider.
A program may use at most 768 MiB of HBM per device.

```python
import jax
import jax.numpy as jnp
from jax import lax

VOCAB_SIZE = 32000
HIDDEN = 2048
BATCH_ROWS = 1
SEQ_LEN = 1024
RMS_EPS = 1e-5


def setup_inputs(seed: int = 0, part: int = 0) -> dict:
    base_key = jax.random.key(seed)
    key_table, key_gain, key_perm, key_ids, key_grad = jax.random.split(base_key, 5)
    popularity = jax.random.permutation(key_perm, VOCAB_SIZE)
    uniform_draws = jax.random.randint(jax.random.fold_in(key_ids, part), (BATCH_ROWS, SEQ_LEN), 1, 1048577)
    ranks = (67108864 // uniform_draws - 64) % VOCAB_SIZE
    token_ids = jnp.take(popularity, ranks).astype(jnp.int32)
    token_ids = token_ids.at[0, 0].set(0).at[BATCH_ROWS - 1, SEQ_LEN - 1].set(VOCAB_SIZE - 1)
    emb_table = jax.random.normal(key_table, (VOCAB_SIZE, HIDDEN), jnp.float32).astype(jnp.bfloat16)
    norm_gain = (1.0 + 0.5 * jax.random.normal(key_gain, (HIDDEN,), jnp.float32)).astype(jnp.bfloat16)
    grad_out = jax.random.normal(jax.random.fold_in(key_grad, part), (BATCH_ROWS, SEQ_LEN, HIDDEN), jnp.float32).astype(jnp.bfloat16)
    return {'token_ids': token_ids, 'emb_table': emb_table, 'norm_gain': norm_gain, 'grad_out': grad_out}


def reference(token_ids, emb_table, norm_gain, grad_out):
    embedded = jnp.take(emb_table, token_ids, axis=0)
    hidden_f32 = embedded.astype(jnp.float32)
    inv_rms = lax.rsqrt(jnp.mean(hidden_f32 * hidden_f32, axis=-1, keepdims=True) + RMS_EPS)
    x_hat = hidden_f32 * inv_rms
    normed = x_hat.astype(jnp.bfloat16) * norm_gain
    grad_f32 = grad_out.astype(jnp.float32)
    grad_gain = jnp.sum(grad_f32 * x_hat, axis=(0, 1))
    grad_hat = grad_f32 * norm_gain.astype(jnp.float32)
    grad_in = inv_rms * (grad_hat - x_hat * jnp.mean(grad_hat * x_hat, axis=-1, keepdims=True))
    grad_rows = grad_in.astype(jnp.bfloat16).astype(jnp.float32).reshape(-1, HIDDEN)
    grad_table = jax.ops.segment_sum(grad_rows, token_ids.reshape(-1), num_segments=VOCAB_SIZE)
    return normed, grad_table, grad_gain
```

```python
import functools

import jax
import jax.numpy as jnp
from jax import lax
from jax.experimental import pallas as pl
from jax.experimental.pallas import tpu as pltpu
from jax.sharding import PartitionSpec as P

RMS_EPS = 1e-5
PAIR_ROWS = 40
MESH = pl.DeviceIdType.MESH
F32 = jnp.float32
BF16 = jnp.bfloat16


def exchange_kernel(n, x_out, dy_out, x_in, dy_in, dg_ref, dg_parts, x_send, x_recv, dy_send, dy_recv, dg_send, dg_recv):
    me = lax.axis_index('tp')
    dp = lax.axis_index('dp')
    hidden = x_out.shape[-1]
    barrier = pltpu.get_barrier_semaphore()
    for step in range(1, n):
        pl.semaphore_signal(barrier, inc=1, device_id=(dp, lax.rem(me + step, n)), device_id_type=MESH)
    pl.semaphore_wait(barrier, n - 1)

    def copies(src, dst, send_sem, recv_sem, step):
        peer = lax.rem(me + step, n)
        return pltpu.make_async_remote_copy(
            src_ref=src.at[peer], dst_ref=dst.at[me], send_sem=send_sem.at[step], recv_sem=recv_sem.at[step],
            device_id=(dp, peer), device_id_type=MESH)

    def arrival(dst, send_sem, recv_sem, step):
        source = lax.rem(me + n - step, n)
        return pltpu.make_async_remote_copy(
            src_ref=dst.at[source], dst_ref=dst.at[source], send_sem=send_sem.at[step], recv_sem=recv_sem.at[step],
            device_id=(dp, source), device_id_type=MESH)

    x_copies = [copies(x_out, x_in, x_send, x_recv, step) for step in range(1, n)]
    for copy in x_copies:
        copy.start()
    dy_copies = [copies(dy_out, dy_in, dy_send, dy_recv, step) for step in range(1, n)]
    for copy in dy_copies:
        copy.start()
    x_in[me] = x_out[me]
    dy_in[me] = dy_out[me]

    def dg_of(block):
        h = x_in[block].astype(F32)
        r = lax.rsqrt(jnp.mean(h * h, axis=-1, keepdims=True) + RMS_EPS)
        return jnp.sum(dy_out[block].astype(F32) * (h * r), axis=0, keepdims=True)

    part = dg_of(me)
    for step in range(1, n):
        arrival(x_in, x_send, x_recv, step).wait_recv()
        part = part + dg_of(lax.rem(me + n - step, n))
    dg_parts[me] = part

    def dg_copy(step):
        peer = lax.rem(me + step, n)
        return pltpu.make_async_remote_copy(
            src_ref=dg_parts.at[me], dst_ref=dg_parts.at[me], send_sem=dg_send.at[step], recv_sem=dg_recv.at[step],
            device_id=(dp, peer), device_id_type=MESH)

    dg_copies = [dg_copy(step) for step in range(1, n)]
    for copy in dg_copies:
        copy.start()
    for step in range(1, n):
        arrival(dy_in, dy_send, dy_recv, step).wait_recv()
    for step in range(1, n):
        arrival(dg_parts, dg_send, dg_recv, step).wait_recv()
    total = dg_parts[0]
    for i in range(1, n):
        total = total + dg_parts[i]
    dg_ref[...] = total
    for copy in x_copies + dy_copies + dg_copies:
        copy.wait_send()


def finish_kernel(zero_rows, target_ref, x_in, slot_ref, x_own, dy_in, g_ref, id_col, id_row, y_ref, de_ref, zeros, sums, zero_sem, row_sem):
    rows = de_ref.shape[0]
    slots = sums.shape[0]
    zeros[...] = jnp.zeros_like(zeros)
    zero_copies = [pltpu.make_async_copy(zeros, de_ref.at[pl.ds(i * zero_rows, zero_rows)], zero_sem.at[i]) for i in range(rows // zero_rows)]
    for copy in zero_copies:
        copy.start()
    gain = g_ref[...]
    gain32 = gain.astype(F32)

    def rms(h):
        return lax.rsqrt(jnp.mean(h * h, axis=-1, keepdims=True) + RMS_EPS)

    positions = y_ref.shape[0]
    pick = (slot_ref[...] == lax.broadcasted_iota(jnp.int32, (positions, slots), 1)).astype(BF16)
    h = jnp.dot(pick, x_in[...], preferred_element_type=F32)
    y_ref[...] = (h * rms(h)).astype(BF16) * gain

    h = x_own[...].astype(F32)
    r = rms(h)
    xh = h * r
    u = dy_in[...].astype(F32) * gain32
    dx = (r * (u - xh * jnp.mean(u * xh, axis=-1, keepdims=True))).astype(BF16)
    same = (id_col[...] == id_row[...]).astype(BF16)
    sums[...] = jnp.dot(same, dx, preferred_element_type=F32)
    for copy in zero_copies:
        copy.wait()

    def row_copy(k):
        return pltpu.make_async_copy(sums.at[pl.ds(k, 1)], de_ref.at[pl.ds(target_ref[k], 1)], row_sem)

    def start(k, _):
        @pl.when(target_ref[k] >= 0)
        def _():
            row_copy(k).start()
        return 0

    def wait(k, _):
        @pl.when(target_ref[k] >= 0)
        def _():
            row_copy(k).wait()
        return 0

    lax.fori_loop(0, slots, start, 0)
    lax.fori_loop(0, slots, wait, 0)


def divisor(rows, most):
    return max(d for d in range(8, most + 1, 8) if rows % d == 0)


def planned(n, cap, ids, table_block, norm_gain, grad_block):
    rows, hidden = table_block.shape
    positions = ids.shape[1]
    me = lax.axis_index('tp')
    before = (lax.broadcasted_iota(jnp.int32, (positions, positions), 0) < lax.broadcasted_iota(jnp.int32, (positions, positions), 1)).astype(jnp.int32)

    def slots_of(mask):
        return jnp.sum(mask.astype(jnp.int32)[:, :, None] * before[None], axis=1)

    local = ids - me * rows
    mine = (local >= 0) & (local < rows)
    slot = slots_of(mine)
    hit = mine[:, None, :] & (slot[:, None, :] == jnp.arange(cap)[None, :, None])
    wanted = jnp.sum(jnp.where(hit, local[:, None, :] + 1, 0), axis=-1).reshape(n * cap) - 1
    x_own = jnp.take(table_block, jnp.maximum(wanted, 0), axis=0)

    my_ids = lax.dynamic_index_in_dim(ids, me, 0, keepdims=True)
    starts = jnp.arange(n, dtype=jnp.int32)[:, None] * rows
    theirs = (my_ids >= starts) & (my_ids < starts + rows)
    their_slot = slots_of(theirs)
    hot = theirs[:, None, :] & (their_slot[:, None, :] == jnp.arange(cap)[None, :, None])
    dy_out = jnp.dot(hot.reshape(n * cap, positions).astype(BF16), grad_block.reshape(positions, hidden))
    slot_col = jnp.sum(jnp.where(theirs, jnp.arange(n)[:, None] * cap + their_slot, 0), axis=0)[:, None]

    earlier = (wanted[None, :] == wanted[:, None]) & (jnp.arange(n * cap)[None, :] < jnp.arange(n * cap)[:, None])
    target = jnp.where(jnp.any(earlier, axis=1), -1, wanted)

    slots_vmem = pltpu.VMEM((n, 1, hidden), F32)
    dma = pltpu.SemaphoreType.DMA((n,))
    x_in, dy_in, dg = pl.pallas_call(
        functools.partial(exchange_kernel, n),
        out_shape=(jax.ShapeDtypeStruct((n, cap, hidden), BF16), jax.ShapeDtypeStruct((n, cap, hidden), BF16), jax.ShapeDtypeStruct((1, hidden), F32)),
        in_specs=[pl.BlockSpec(memory_space=pltpu.VMEM)] * 2,
        out_specs=(pl.BlockSpec(memory_space=pltpu.VMEM),) * 3,
        scratch_shapes=[slots_vmem] + [dma] * 6,
        compiler_params=pltpu.CompilerParams(collective_id=cap, has_side_effects=True, vmem_limit_bytes=60 * 2**20),
        name=f'exchange{cap}',
    )(x_own.reshape(n, cap, hidden), dy_out.reshape(n, cap, hidden))

    zero_rows = divisor(rows, 256)
    y, grad_table = pl.pallas_call(
        functools.partial(finish_kernel, zero_rows),
        out_shape=(jax.ShapeDtypeStruct((positions, hidden), BF16), jax.ShapeDtypeStruct((rows, hidden), F32)),
        in_specs=[pl.BlockSpec(memory_space=pltpu.SMEM)] + [pl.BlockSpec(memory_space=pltpu.VMEM)] * 7,
        out_specs=(pl.BlockSpec(memory_space=pltpu.VMEM), pl.BlockSpec(memory_space=pl.ANY)),
        scratch_shapes=[pltpu.VMEM((zero_rows, hidden), F32), pltpu.VMEM((n * cap, hidden), F32), pltpu.SemaphoreType.DMA((rows // zero_rows,)), pltpu.SemaphoreType.DMA],
        compiler_params=pltpu.CompilerParams(vmem_limit_bytes=60 * 2**20),
        name=f'finish{cap}',
    )(target, x_in.reshape(n * cap, hidden), slot_col, x_own, dy_in.reshape(n * cap, hidden), norm_gain[None], wanted[:, None], wanted[None])
    return y.reshape(grad_block.shape), grad_table, dg.reshape(hidden)


def device_step(n, token_ids, table_block, norm_gain, grad_block):
    positions = grad_block.shape[0] * grad_block.shape[1]
    rows = table_block.shape[0]
    ids = token_ids.reshape(n, positions)
    owners = jnp.sum((ids[:, None, :] >= jnp.arange(1, n, dtype=jnp.int32)[None, :, None] * rows).astype(jnp.int32), axis=1)
    counts = jnp.sum((owners[:, None, :] == jnp.arange(n)[None, :, None]).astype(jnp.int32), axis=-1)
    cap = min(PAIR_ROWS, positions)
    args = (ids, table_block, norm_gain, grad_block)
    if cap == positions:
        return planned(n, cap, *args)
    return lax.cond(jnp.max(counts) <= cap, functools.partial(planned, n, cap), functools.partial(planned, n, positions), *args)


def solution(mesh):
    return jax.shard_map(functools.partial(device_step, mesh.shape['tp']), mesh=mesh, in_specs=(P('dp', None), P('tp', None), P(None), P('dp', 'tp', None)), out_specs=(P('dp', 'tp', None), P(('dp', 'tp'), None), P('dp')), check_vma=False)
```

```python
import functools

import jax
import jax.numpy as jnp
from jax import lax
from jax.experimental import pallas as pl
from jax.experimental.pallas import tpu as pltpu
from jax.sharding import PartitionSpec as P

RMS_EPS = 1e-5
CORES = 2
X_ROWS = 40
DY_ROWS = 56
ZERO_FIRST = 12
MESH = pl.DeviceIdType.MESH
F32 = jnp.float32
BF16 = jnp.bfloat16
I32 = jnp.int32
NT = (((1,), (1,)), ((), ()))
TN = (((0,), (0,)), ((), ()))
LIMIT = 60 * 2**20


def iota(shape, dim):
    return lax.broadcasted_iota(I32, shape, dim)


def divisor(rows, most):
    return max(d for d in range(8, most + 1, 8) if rows % d == 0)


def rms(h):
    return lax.rsqrt(jnp.mean(h * h, axis=-1, keepdims=True) + RMS_EPS)


def column(row):
    size = row.shape[1]
    return jnp.sum(jnp.where(iota((size, size), 0) == iota((size, size), 1), row, 0.0), axis=1, keepdims=True)


def firsts(even, odd):
    size = even.shape[1]
    before = iota((size, size), 0) < iota((size, size), 1)
    even_col, odd_col = column(even), column(odd)
    even_dup = jnp.where((even_col == even) & before, 1.0, 0.0)
    odd_dup = jnp.where((even_col == odd) | ((odd_col == odd) & before), 1.0, 0.0)
    return 1.0 - jnp.max(even_dup, axis=0, keepdims=True), 1.0 - jnp.max(odd_dup, axis=0, keepdims=True)


def one_hots(mask, offset, cap):
    size = mask.shape[1]
    before = (iota((size, size), 0) < iota((size, size), 1)).astype(BF16)
    rank = jnp.dot(mask.astype(BF16), before, preferred_element_type=F32)
    if offset is not None:
        rank = rank + offset
    rank = jnp.where(mask > 0.0, rank, -1.0).astype(I32)
    slots = iota((cap, size), 0)
    return jnp.concatenate([jnp.where(rank[i:i + 1] == slots, 1.0, 0.0) for i in range(mask.shape[0])], axis=0)


def halves(ids):
    code = ids + 1
    return (code >> 8).astype(F32), (code & 255).astype(F32)


def unique_lists(even_mask, odd_mask, even_code, odd_code, cap):
    even_hot = one_hots(even_mask, None, cap)
    odd_hot = one_hots(odd_mask, jnp.sum(even_mask, axis=1, keepdims=True), cap)
    return (lax.dot_general(even_code.astype(BF16), even_hot.astype(BF16), NT, preferred_element_type=F32)
            + lax.dot_general(odd_code.astype(BF16), odd_hot.astype(BF16), NT, preferred_element_type=F32))


def within(ids, low, high):
    return jnp.where((ids >= low) & (ids < high), 1.0, 0.0)


def prepare_kernel(n, zero_rows, first, ids_ref, table_ref, de_ref, x_ref, list_ref, target_ref, flag_ref,
                   zeros, slabs, local, local_smem, targets, zero_sem, slab_sem, small_sem):
    me = lax.axis_index('tp')
    rows = de_ref.shape[0]
    chips = n // CORES
    slots = chips * X_ROWS
    zeros[...] = jnp.zeros_like(zeros)
    zero_copies = [pltpu.make_async_copy(zeros, de_ref.at[pl.ds(i * zero_rows, zero_rows)], zero_sem.at[i]) for i in range(first)]
    for copy in zero_copies:
        copy.start()

    ids = ids_ref[...]
    even = jnp.concatenate([ids[CORES * d:CORES * d + 1] for d in range(chips)], axis=0)
    odd = jnp.concatenate([ids[CORES * d + 1:CORES * d + 2] for d in range(chips)], axis=0)
    even_f, odd_f = even.astype(F32), odd.astype(F32)
    flags = [firsts(even_f[d:d + 1], odd_f[d:d + 1]) for d in range(chips)]
    even_first = jnp.concatenate([f[0] for f in flags], axis=0)
    odd_first = jnp.concatenate([f[1] for f in flags], axis=0)
    even_mine = within(even, me * rows, me * rows + rows) * even_first
    odd_mine = within(odd, me * rows, me * rows + rows) * odd_first
    even_code = jnp.concatenate(halves(even), axis=0)
    odd_code = jnp.concatenate(halves(odd), axis=0)
    product = unique_lists(even_mine, odd_mine, even_code, odd_code, X_ROWS)
    row_of, slot_of = iota(product.shape, 0), iota(product.shape, 1)
    own_block = (row_of % chips) == (slot_of // X_ROWS)
    wanted = jnp.sum(jnp.where(own_block, product * jnp.where(row_of < chips, 256.0, 1.0), 0.0), axis=0, keepdims=True) - 1.0
    row_in_block = jnp.maximum(wanted.astype(I32) - me * rows, 0)
    local[...] = jnp.broadcast_to(row_in_block, local.shape)
    to_smem = pltpu.make_async_copy(local, local_smem, small_sem.at[0])
    to_smem.start()
    to_smem.wait()

    def slab_copy(k):
        base = pl.multiple_of((local_smem[0, k] // 8) * 8, 8)
        return pltpu.make_async_copy(table_ref.at[pl.ds(base, 8)], slabs.at[k], slab_sem.at[k // X_ROWS])

    for d in range(chips):
        def start(s, _, d=d):
            slab_copy(d * X_ROWS + s).start()
            return 0
        lax.fori_loop(0, X_ROWS, start, 0)

    wanted_col = column(wanted)
    earlier = iota((slots, slots), 0) < iota((slots, slots), 1)
    repeated = jnp.max(jnp.where((wanted_col == wanted) & earlier, 1.0, 0.0), axis=0, keepdims=True)
    first_list = jnp.where(repeated > 0.0, -1.0, wanted)
    list_ref[...] = jnp.broadcast_to(first_list, list_ref.shape)
    targets[...] = jnp.broadcast_to(jnp.where(first_list >= 0.0, first_list - (me * rows).astype(F32), -1.0).astype(I32), targets.shape)
    out_targets = pltpu.make_async_copy(targets, target_ref, small_sem.at[1])
    out_targets.start()

    most = jnp.zeros((1, 1), F32)
    for i in range(n):
        held = within(even, i * rows, i * rows + rows) * even_first + within(odd, i * rows, i * rows + rows) * odd_first
        most = jnp.maximum(most, jnp.max(jnp.sum(held, axis=1, keepdims=True) * (1.0 / X_ROWS), axis=0, keepdims=True))
    for c in range(chips):
        held = jnp.sum(within(ids, c * CORES * rows, (c + 1) * CORES * rows), axis=1, keepdims=True)
        most = jnp.maximum(most, jnp.max(held * (1.0 / DY_ROWS), axis=0, keepdims=True))
    flag_ref[...] = jnp.broadcast_to(jnp.where(most > 1.0005, 0, 1), flag_ref.shape)

    remainder = column((row_in_block % 8).astype(F32)).astype(I32)
    hot_row, hot_col = iota((X_ROWS, X_ROWS * 8), 0), iota((X_ROWS, X_ROWS * 8), 1)
    for d in range(chips):
        def wait(s, _, d=d):
            pltpu.make_async_copy(table_ref.at[pl.ds(0, 8)], slabs.at[d * X_ROWS + s], slab_sem.at[d]).wait()
            return 0
        lax.fori_loop(0, X_ROWS, wait, 0)
        pick = jnp.where(hot_col == hot_row * 8 + remainder[d * X_ROWS:(d + 1) * X_ROWS], 1.0, 0.0).astype(BF16)
        block = slabs[pl.ds(d * X_ROWS, X_ROWS)].reshape(X_ROWS * 8, x_ref.shape[-1])
        x_ref[d] = jnp.dot(pick, block, preferred_element_type=F32).astype(BF16)
    out_targets.wait()
    for copy in zero_copies:
        copy.wait()


def exchange_kernel(n, rows, ids_ref, x_hbm, dy_hbm, xpos_ref, dy_all, dg_ref, x_own, dy_own, x_in, dy_out, dy_in, dg_parts,
                    local_sem, x_send, x_recv, xf_send, xf_recv, dy_send, dy_recv, dyf_send, dyf_recv, dg_send, dg_recv, out_sem):
    me = lax.axis_index('tp')
    dp = lax.axis_index('dp')
    chips = n // CORES
    chip = me // CORES
    core = me % CORES
    partner = chip * CORES + 1 - core
    barrier = pltpu.get_barrier_semaphore()
    for step in range(1, n):
        pl.semaphore_signal(barrier, inc=1, device_id=(dp, lax.rem(me + step, n)), device_id_type=MESH)
    load_dy = pltpu.make_async_copy(dy_hbm, dy_own, local_sem.at[0])
    load_dy.start()
    load_x = pltpu.make_async_copy(x_hbm, x_own, local_sem.at[1])
    load_x.start()

    my_ids = ids_ref[pl.ds(me, 1)]
    chip_masks = jnp.concatenate([within(my_ids, c * CORES * rows, (c + 1) * CORES * rows) for c in range(chips)], axis=0)
    dy_hot = one_hots(chip_masks, None, DY_ROWS).astype(BF16)
    load_dy.wait()
    for c in range(chips):
        dy_out[c] = jnp.dot(dy_hot[c * DY_ROWS:(c + 1) * DY_ROWS], dy_own[...], preferred_element_type=F32).astype(BF16)
    load_x.wait()
    pl.semaphore_wait(barrier, n - 1)

    def remote(src, dst, send_sem, recv_sem, device):
        return pltpu.make_async_remote_copy(src_ref=src, dst_ref=dst, send_sem=send_sem, recv_sem=recv_sem, device_id=(dp, device), device_id_type=MESH)

    sent = []

    def send_all(src, dst, send_sem, recv_sem, forward_send, forward_recv):
        for step in range(1, chips):
            there = lax.rem(chip + step, chips)
            copy = remote(src.at[there], dst.at[me], send_sem.at[step], recv_sem.at[step], there * CORES + core)
            copy.start()
            sent.append(copy)
        copy = remote(src.at[chip], dst.at[me], forward_send.at[0], forward_recv.at[0], partner)
        copy.start()
        sent.append(copy)
        dst[me] = src[chip]

    def source(step):
        return lax.rem(chip + chips - step, chips) * CORES

    def receive(dst, send_sem, recv_sem, forward_send, forward_recv, step):
        block = dst.at[source(step) + core]
        remote(block, block, send_sem.at[step], recv_sem.at[step], partner).wait_recv()
        copy = remote(block, block, forward_send.at[step], forward_recv.at[step], partner)
        copy.start()
        sent.append(copy)

    def receive_forwarded(dst, forward_send, forward_recv, step):
        block = dst.at[source(step) + 1 - core]
        remote(block, block, forward_send.at[step], forward_recv.at[step], partner).wait_recv()

    x_sems = (x_send, x_recv, xf_send, xf_recv)
    dy_sems = (dy_send, dy_recv, dyf_send, dyf_recv)
    send_all(x_own, x_in, *x_sems)
    send_all(dy_out, dy_in, *dy_sems)

    even, odd = ids_ref[pl.ds(chip * CORES, 1)], ids_ref[pl.ds(chip * CORES + 1, 1)]
    even_first, odd_first = firsts(even.astype(F32), odd.astype(F32))
    even_mask = jnp.concatenate([within(even, i * rows, (i + 1) * rows) for i in range(n)], axis=0) * even_first
    odd_mask = jnp.concatenate([within(odd, i * rows, (i + 1) * rows) for i in range(n)], axis=0) * odd_first
    pad = jnp.zeros((6, even.shape[1]), F32)
    even_code = jnp.concatenate(halves(even) + (pad,), axis=0)
    odd_code = jnp.concatenate(halves(odd) + (pad,), axis=0)
    product = unique_lists(even_mask, odd_mask, even_code, odd_code, X_ROWS)
    held = product[0:1] * 256.0 + product[1:2] - 1.0
    pick = jnp.where(column(my_ids.astype(F32)) == held, 1.0, 0.0).astype(BF16)

    order = [1, chips - 1] + list(range(2, chips - 1))
    for step in order:
        receive(x_in, *x_sems, step)
    for step in [0] + order:
        receive_forwarded(x_in, xf_send, xf_recv, step)
    hidden = xpos_ref.shape[-1]
    h = jnp.dot(pick, x_in[...].reshape(n * X_ROWS, hidden), preferred_element_type=F32)
    xpos_ref[...] = h.astype(BF16)
    dg_parts[me] = jnp.sum(dy_own[...].astype(F32) * (h * rms(h)), axis=0, keepdims=True)
    for step in range(1, n):
        copy = remote(dg_parts.at[me], dg_parts.at[me], dg_send.at[step], dg_recv.at[step], lax.rem(me + step, n))
        copy.start()
        sent.append(copy)

    outs = []

    def put(block):
        copy = pltpu.make_async_copy(dy_in.at[block], dy_all.at[block], out_sem.at[len(outs)])
        copy.start()
        outs.append(copy)

    put(me)
    for step in order:
        receive(dy_in, *dy_sems, step)
        put(source(step) + core)
    for step in [0] + order:
        receive_forwarded(dy_in, dyf_send, dyf_recv, step)
        put(source(step) + 1 - core)
    for step in range(1, n):
        block = dg_parts.at[lax.rem(me + n - step, n)]
        remote(block, block, dg_send.at[step], dg_recv.at[step], partner).wait_recv()
    total = dg_parts[0]
    for i in range(1, n):
        total = total + dg_parts[i]
    dg_ref[...] = total
    for copy in sent:
        copy.wait_send()
    for copy in outs:
        copy.wait()


def finish_kernel(n, zero_rows, first, target_ref, ids_ref, list_ref, xpos_ref, x_ref, dy_ref, g_ref, de_in, y_ref, de_ref,
                  zeros, dx_all, picks, sums, zero_sem, row_sem):
    me = lax.axis_index('tp')
    rows = de_ref.shape[0]
    slots = sums.shape[0]
    hidden = sums.shape[1]
    chip = me // CORES
    zeros[...] = jnp.zeros_like(zeros)
    zero_copies = [pltpu.make_async_copy(zeros, de_ref.at[pl.ds(i * zero_rows, zero_rows)], zero_sem.at[i]) for i in range(first, rows // zero_rows)]
    for copy in zero_copies:
        copy.start()
    gain = g_ref[...]
    gain32 = gain.astype(F32)
    h = xpos_ref[...].astype(F32)
    y_ref[...] = (h * rms(h)).astype(BF16) * gain

    ids = ids_ref[...]
    mask = within(ids, chip * CORES * rows, (chip + 1) * CORES * rows)
    hots = one_hots(mask, None, DY_ROWS)
    own_list = list_ref[0:1]
    x_own = x_ref[...].reshape(slots, hidden)
    for i in range(n):
        code = (ids[i:i + 1] + 2).astype(F32)
        row_ids = jnp.sum(hots[i * DY_ROWS:(i + 1) * DY_ROWS] * code, axis=1, keepdims=True) - 2.0
        picks[pl.ds(i * DY_ROWS, DY_ROWS)] = jnp.where(row_ids == own_list, 1.0, 0.0)

    def body(i, _):
        part = pl.ds(pl.multiple_of(i * DY_ROWS, DY_ROWS), DY_ROWS)
        h = jnp.dot(picks[part].astype(BF16), x_own, preferred_element_type=F32)
        r = rms(h)
        xh = h * r
        u = dy_ref[i].astype(F32) * gain32
        dx_all[part] = r * (u - xh * jnp.mean(u * xh, axis=-1, keepdims=True))
        return 0

    lax.fori_loop(0, n, body, 0)
    sums[...] = lax.dot_general(picks[...].astype(BF16), dx_all[...].astype(BF16), TN, preferred_element_type=F32)
    for copy in zero_copies:
        copy.wait()

    def row_copy(k):
        return pltpu.make_async_copy(sums.at[pl.ds(k, 1)], de_ref.at[pl.ds(target_ref[0, k], 1)], row_sem)

    def start(k, _):
        @pl.when(target_ref[0, k] >= 0)
        def _():
            row_copy(k).start()
        return 0

    def wait(k, _):
        @pl.when(target_ref[0, k] >= 0)
        def _():
            row_copy(k).wait()
        return 0

    lax.fori_loop(0, slots, start, 0)
    lax.fori_loop(0, slots, wait, 0)


def vmem():
    return pl.BlockSpec(memory_space=pltpu.VMEM)


def smem():
    return pl.BlockSpec(memory_space=pltpu.SMEM)


def anywhere():
    return pl.BlockSpec(memory_space=pl.ANY)


def dma(*shape):
    return pltpu.SemaphoreType.DMA(shape)


def fast_path(n, zero_rows, first, ids, grad_table, x_own, own_list, target, table_block, norm_gain, grad_block):
    rows, hidden = table_block.shape
    positions = ids.shape[1]
    chips = n // CORES
    slots = chips * X_ROWS
    xpos, dy_all, dg = pl.pallas_call(
        functools.partial(exchange_kernel, n, rows),
        out_shape=(jax.ShapeDtypeStruct((positions, hidden), BF16), jax.ShapeDtypeStruct((n, DY_ROWS, hidden), BF16), jax.ShapeDtypeStruct((1, hidden), F32)),
        in_specs=[vmem(), anywhere(), anywhere()],
        out_specs=(vmem(), anywhere(), vmem()),
        scratch_shapes=[
            pltpu.VMEM((chips, X_ROWS, hidden), BF16), pltpu.VMEM((positions, hidden), BF16),
            pltpu.VMEM((n, X_ROWS, hidden), BF16), pltpu.VMEM((chips, DY_ROWS, hidden), BF16), pltpu.VMEM((n, DY_ROWS, hidden), BF16),
            pltpu.VMEM((n, 1, hidden), F32), dma(2)] + [dma(chips)] * 8 + [dma(n)] * 3,
        compiler_params=pltpu.CompilerParams(collective_id=0, has_side_effects=True, vmem_limit_bytes=LIMIT),
        name='exchange_lists',
    )(ids, x_own, grad_block.reshape(positions, hidden))
    y, grad_table = pl.pallas_call(
        functools.partial(finish_kernel, n, zero_rows, first),
        out_shape=(jax.ShapeDtypeStruct((positions, hidden), BF16), jax.ShapeDtypeStruct((rows, hidden), F32)),
        in_specs=[smem()] + [vmem()] * 6 + [anywhere()],
        out_specs=(vmem(), anywhere()),
        input_output_aliases={7: 1},
        scratch_shapes=[
            pltpu.VMEM((zero_rows, hidden), F32), pltpu.VMEM((n * DY_ROWS, hidden), F32), pltpu.VMEM((n * DY_ROWS, slots), F32),
            pltpu.VMEM((slots, hidden), F32), dma(rows // zero_rows), pltpu.SemaphoreType.DMA],
        compiler_params=pltpu.CompilerParams(vmem_limit_bytes=LIMIT),
        name='finish_lists',
    )(target, ids, own_list, xpos, x_own, dy_all, norm_gain[None], grad_table)
    return y.reshape(grad_block.shape), grad_table, dg.reshape(hidden)


def pair_exchange_kernel(n, x_out, dy_out, x_in, dy_in, dg_ref, dg_parts, x_send, x_recv, dy_send, dy_recv, dg_send, dg_recv):
    me = lax.axis_index('tp')
    dp = lax.axis_index('dp')
    barrier = pltpu.get_barrier_semaphore()
    for step in range(1, n):
        pl.semaphore_signal(barrier, inc=1, device_id=(dp, lax.rem(me + step, n)), device_id_type=MESH)
    pl.semaphore_wait(barrier, n - 1)

    def copies(src, dst, send_sem, recv_sem, step):
        peer = lax.rem(me + step, n)
        return pltpu.make_async_remote_copy(
            src_ref=src.at[peer], dst_ref=dst.at[me], send_sem=send_sem.at[step], recv_sem=recv_sem.at[step],
            device_id=(dp, peer), device_id_type=MESH)

    def arrival(dst, send_sem, recv_sem, step):
        source = lax.rem(me + n - step, n)
        return pltpu.make_async_remote_copy(
            src_ref=dst.at[source], dst_ref=dst.at[source], send_sem=send_sem.at[step], recv_sem=recv_sem.at[step],
            device_id=(dp, source), device_id_type=MESH)

    x_copies = [copies(x_out, x_in, x_send, x_recv, step) for step in range(1, n)]
    for copy in x_copies:
        copy.start()
    dy_copies = [copies(dy_out, dy_in, dy_send, dy_recv, step) for step in range(1, n)]
    for copy in dy_copies:
        copy.start()
    x_in[me] = x_out[me]
    dy_in[me] = dy_out[me]

    def dg_of(block):
        h = x_in[block].astype(F32)
        return jnp.sum(dy_out[block].astype(F32) * (h * rms(h)), axis=0, keepdims=True)

    for step in range(1, n):
        arrival(x_in, x_send, x_recv, step).wait_recv()
    dg_parts[me] = lax.fori_loop(1, n, lambda i, total: total + dg_of(i), dg_of(0))

    def dg_copy(step):
        return pltpu.make_async_remote_copy(
            src_ref=dg_parts.at[me], dst_ref=dg_parts.at[me], send_sem=dg_send.at[step], recv_sem=dg_recv.at[step],
            device_id=(dp, lax.rem(me + step, n)), device_id_type=MESH)

    dg_copies = [dg_copy(step) for step in range(1, n)]
    for copy in dg_copies:
        copy.start()
    for step in range(1, n):
        arrival(dy_in, dy_send, dy_recv, step).wait_recv()
    for step in range(1, n):
        arrival(dg_parts, dg_send, dg_recv, step).wait_recv()
    total = dg_parts[0]
    for i in range(1, n):
        total = total + dg_parts[i]
    dg_ref[...] = total
    for copy in x_copies + dy_copies + dg_copies:
        copy.wait_send()


def any_path(n, ids, table_block, norm_gain, grad_block):
    rows, hidden = table_block.shape
    positions = ids.shape[1]
    cap = positions
    me = lax.axis_index('tp')
    before = (iota((positions, positions), 0) < iota((positions, positions), 1)).astype(I32)

    def slots_of(mask):
        return jnp.sum(mask.astype(I32)[:, :, None] * before[None], axis=1)

    local = ids - me * rows
    mine = (local >= 0) & (local < rows)
    slot = slots_of(mine)
    hit = mine[:, None, :] & (slot[:, None, :] == jnp.arange(cap)[None, :, None])
    wanted = jnp.sum(jnp.where(hit, local[:, None, :] + 1, 0), axis=-1).reshape(n * cap) - 1
    x_own = jnp.take(table_block, jnp.maximum(wanted, 0), axis=0)
    my_ids = lax.dynamic_index_in_dim(ids, me, 0, keepdims=True)
    starts = jnp.arange(n, dtype=I32)[:, None] * rows
    theirs = (my_ids >= starts) & (my_ids < starts + rows)
    their_slot = slots_of(theirs)
    hot = theirs[:, None, :] & (their_slot[:, None, :] == jnp.arange(cap)[None, :, None])
    dy_out = jnp.dot(hot.reshape(n * cap, positions).astype(BF16), grad_block.reshape(positions, hidden))
    slot_of = jnp.sum(jnp.where(theirs, jnp.arange(n)[:, None] * cap + their_slot, 0), axis=0)
    x_in, dy_in, dg = pl.pallas_call(
        functools.partial(pair_exchange_kernel, n),
        out_shape=(jax.ShapeDtypeStruct((n, cap, hidden), BF16), jax.ShapeDtypeStruct((n, cap, hidden), BF16), jax.ShapeDtypeStruct((1, hidden), F32)),
        in_specs=[vmem(), vmem()],
        out_specs=(vmem(), vmem(), vmem()),
        scratch_shapes=[pltpu.VMEM((n, 1, hidden), F32)] + [dma(n)] * 6,
        compiler_params=pltpu.CompilerParams(collective_id=1, has_side_effects=True, vmem_limit_bytes=LIMIT),
        name='exchange_pairs',
    )(x_own.reshape(n, cap, hidden), dy_out.reshape(n, cap, hidden))
    h = jnp.take(x_in.reshape(n * cap, hidden), slot_of, axis=0).astype(F32)
    y = (h * rms(h)).astype(BF16) * norm_gain
    h = x_own.astype(F32)
    r = rms(h)
    xh = h * r
    u = dy_in.reshape(n * cap, hidden).astype(F32) * norm_gain.astype(F32)
    dx = (r * (u - xh * jnp.mean(u * xh, axis=-1, keepdims=True))).astype(BF16)
    grad_table = jax.ops.segment_sum(dx.astype(F32), jnp.where(wanted >= 0, wanted, rows), num_segments=rows)
    return y.reshape(grad_block.shape), grad_table, dg.reshape(hidden)


def device_step(n, token_ids, table_block, norm_gain, grad_block):
    positions = grad_block.shape[0] * grad_block.shape[1]
    rows, hidden = table_block.shape
    ids = token_ids.reshape(n, positions)
    chips = n // CORES
    slots = chips * X_ROWS
    zero_rows = divisor(rows, 256)
    first = min(ZERO_FIRST, rows // zero_rows)
    grad_table, x_own, own_list, target, flag = pl.pallas_call(
        functools.partial(prepare_kernel, n, zero_rows, first),
        out_shape=(jax.ShapeDtypeStruct((rows, hidden), F32), jax.ShapeDtypeStruct((chips, X_ROWS, hidden), BF16),
                   jax.ShapeDtypeStruct((8, slots), F32), jax.ShapeDtypeStruct((8, slots), I32), jax.ShapeDtypeStruct((8, 128), I32)),
        in_specs=[vmem(), anywhere()],
        out_specs=(anywhere(), vmem(), vmem(), anywhere(), vmem()),
        scratch_shapes=[
            pltpu.VMEM((zero_rows, hidden), F32), pltpu.VMEM((slots, 8, hidden), BF16), pltpu.VMEM((8, slots), I32), pltpu.SMEM((8, slots), I32),
            pltpu.VMEM((8, slots), I32), dma(first), dma(chips), dma(2)],
        compiler_params=pltpu.CompilerParams(vmem_limit_bytes=LIMIT),
        name='prepare',
    )(ids, table_block)

    def fast(ids, grad_table, x_own, own_list, target, *rest):
        return fast_path(n, zero_rows, first, ids, grad_table, x_own, own_list, target, *rest)

    def slow(ids, grad_table, x_own, own_list, target, *rest):
        return any_path(n, ids, *rest)

    return lax.cond(flag[0, 0] > 0, fast, slow, ids, grad_table, x_own, own_list, target, table_block, norm_gain, grad_block)


def solution(mesh):
    return jax.shard_map(functools.partial(device_step, mesh.shape['tp']), mesh=mesh, in_specs=(P('dp', None), P('tp', None), P(None), P('dp', 'tp', None)), out_specs=(P('dp', 'tp', None), P(('dp', 'tp'), None), P('dp')), check_vma=False)
```

```python
import functools

import jax
import jax.numpy as jnp
from jax import lax
from jax.experimental import pallas as pl
from jax.experimental.pallas import tpu as pltpu
from jax.sharding import PartitionSpec as P

RMS_EPS = 1e-5
CORES = 2
X_ROWS = 40
DY_ROWS = 56
ZERO_ROWS = 80
MESH = pl.DeviceIdType.MESH
F32 = jnp.float32
BF16 = jnp.bfloat16
I32 = jnp.int32
NT = (((1,), (1,)), ((), ()))
TN = (((0,), (0,)), ((), ()))
LIMIT = 60 * 2**20


def iota(shape, dim):
    return lax.broadcasted_iota(I32, shape, dim)


def divisor(rows, most):
    return max(d for d in range(8, most + 1, 8) if rows % d == 0)


def rms(h):
    return lax.rsqrt(jnp.mean(h * h, axis=-1, keepdims=True) + RMS_EPS)


def column(row):
    size = row.shape[1]
    return jnp.sum(jnp.where(iota((size, size), 0) == iota((size, size), 1), row, 0.0), axis=1, keepdims=True)


def firsts(even, odd):
    size = even.shape[1]
    before = iota((size, size), 0) < iota((size, size), 1)
    even_col, odd_col = column(even), column(odd)
    even_dup = jnp.where((even_col == even) & before, 1.0, 0.0)
    odd_dup = jnp.where((even_col == odd) | ((odd_col == odd) & before), 1.0, 0.0)
    return 1.0 - jnp.max(even_dup, axis=0, keepdims=True), 1.0 - jnp.max(odd_dup, axis=0, keepdims=True)


def one_hots(mask, offset, cap):
    size = mask.shape[1]
    before = (iota((size, size), 0) < iota((size, size), 1)).astype(BF16)
    rank = jnp.dot(mask.astype(BF16), before, preferred_element_type=F32)
    if offset is not None:
        rank = rank + offset
    rank = jnp.where(mask > 0.0, rank, -1.0).astype(I32)
    slots = iota((cap, size), 0)
    return jnp.concatenate([jnp.where(rank[i:i + 1] == slots, 1.0, 0.0) for i in range(mask.shape[0])], axis=0)


def halves(ids):
    code = ids + 1
    return (code >> 8).astype(F32), (code & 255).astype(F32)


def unique_lists(even_mask, odd_mask, even_code, odd_code, cap):
    even_hot = one_hots(even_mask, None, cap)
    odd_hot = one_hots(odd_mask, jnp.sum(even_mask, axis=1, keepdims=True), cap)
    return (lax.dot_general(even_code.astype(BF16), even_hot.astype(BF16), NT, preferred_element_type=F32)
            + lax.dot_general(odd_code.astype(BF16), odd_hot.astype(BF16), NT, preferred_element_type=F32))


def wide(lines):
    lines = lines.astype(F32)
    return jnp.concatenate([lines[i:i + 1] for i in range(lines.shape[0])], axis=1)


def within(ids, low, high):
    return jnp.where((ids >= low) & (ids < high), 1.0, 0.0)


def exchange_kernel(n, rows, ids_ref, table_hbm, dy_own, g_ref, xpos_ref, sums_ref, dg_ref, target_ref, over_ref,
                    table, slabs, local, local_smem, x_own, x_in, dy_out, dy_in, picks, spots, dx_all, dg_parts,
                    table_sem, small_sem, x_send, x_recv, xf_send, xf_recv, dy_send, dy_recv, dyf_send, dyf_recv, dg_send, dg_recv):
    chips = n // CORES
    me = lax.axis_index('tp')
    dp = lax.axis_index('dp')
    chip = me // CORES
    core = me % CORES
    partner = chip * CORES + 1 - core
    slots, hidden = sums_ref.shape
    barrier = pltpu.get_barrier_semaphore()
    for step in range(1, n):
        pl.semaphore_signal(barrier, inc=1, device_id=(dp, lax.rem(me + step, n)), device_id_type=MESH)
    pieces = table_sem.shape[0]
    piece = table_hbm.shape[0] // pieces
    table_copies = [pltpu.make_async_copy(table_hbm.at[pl.ds(i * piece, piece)], table.at[pl.ds(i * piece, piece)], table_sem.at[i]) for i in range(pieces)]
    for copy in table_copies:
        copy.start()

    def remote(src, dst, send_sem, recv_sem, device):
        return pltpu.make_async_remote_copy(src_ref=src, dst_ref=dst, send_sem=send_sem, recv_sem=recv_sem, device_id=(dp, device), device_id_type=MESH)

    sent = []

    def send(*args):
        copy = remote(*args)
        copy.start()
        sent.append(copy)

    def source(step):
        return lax.rem(chip + chips - step, chips)

    def device_at(step):
        return lax.rem(chip + step, chips) * CORES + core

    order = [1, chips - 1] + list(range(2, chips - 1))
    low = me * rows

    my_ids = ids_ref[pl.ds(me, 1)]
    near = [lax.rem(chip + step, chips) for step in range(chips)]
    masks = jnp.concatenate([within(my_ids, c * CORES * rows, (c + 1) * CORES * rows) for c in near], axis=0)
    hots = one_hots(masks, None, DY_ROWS).astype(BF16)
    for step in range(chips):
        dy_out[step] = jnp.dot(hots[step * DY_ROWS:(step + 1) * DY_ROWS], dy_own[...], preferred_element_type=F32).astype(BF16)
    pl.semaphore_wait(barrier, n - 1)
    for step in order:
        send(dy_out.at[step], dy_in.at[me], dy_send.at[step], dy_recv.at[step], device_at(step))
    send(dy_out.at[0], dy_in.at[me], dyf_send.at[0], dyf_recv.at[0], partner)
    dy_in[me] = dy_out[0]

    even = jnp.concatenate([ids_ref[pl.ds(c * CORES, 1)] for c in near], axis=0)
    odd = jnp.concatenate([ids_ref[pl.ds(c * CORES + 1, 1)] for c in near], axis=0)
    near_even, near_odd = even, odd
    even_f, odd_f = even.astype(F32), odd.astype(F32)
    flags = [firsts(even_f[d:d + 1], odd_f[d:d + 1]) for d in range(chips)]
    even_first = jnp.concatenate([f[0] for f in flags], axis=0)
    odd_first = jnp.concatenate([f[1] for f in flags], axis=0)
    even_code = jnp.concatenate(halves(even), axis=0)
    odd_code = jnp.concatenate(halves(odd), axis=0)
    product = unique_lists(within(even, low, low + rows) * even_first, within(odd, low, low + rows) * odd_first, even_code, odd_code, X_ROWS)
    row_of, slot_of = iota(product.shape, 0), iota(product.shape, 1)
    own_block = (row_of % chips) == (slot_of // X_ROWS)
    wanted = jnp.sum(jnp.where(own_block, product * jnp.where(row_of < chips, 256.0, 1.0), 0.0), axis=0, keepdims=True) - 1.0
    row_in_block = jnp.clip(wanted.astype(I32) - low, 0, rows - 1)
    local[...] = jnp.broadcast_to(row_in_block >> 3, local.shape)
    to_smem = pltpu.make_async_copy(local, local_smem, small_sem)
    to_smem.start()
    remainder = column((row_in_block & 7).astype(F32)).astype(I32)
    wanted_col = column(wanted)
    earlier = iota((slots, slots), 0) < iota((slots, slots), 1)
    repeated = jnp.max(jnp.where((wanted_col == wanted) & earlier, 1.0, 0.0), axis=0, keepdims=True)
    first_list = jnp.where(repeated > 0.0, -1.0, wanted)
    hot_row, hot_col = iota((X_ROWS, X_ROWS * 8), 0), iota((X_ROWS, X_ROWS * 8), 1)
    for copy in table_copies:
        copy.wait()
    to_smem.wait()
    for step in order + [0]:
        def load(s, _, base=step * X_ROWS):
            for j in range(8):
                k = s * 8 + j
                slabs[k] = table[jnp.clip(local_smem[0, base + k], 0, table.shape[0] - 1)]
            return 0
        lax.fori_loop(0, X_ROWS // 8, load, 0)
        pick = jnp.where(hot_col == hot_row * 8 + remainder[step * X_ROWS:(step + 1) * X_ROWS], 1.0, 0.0).astype(BF16)
        x_own[step] = jnp.dot(pick, slabs[...].reshape(X_ROWS * 8, hidden), preferred_element_type=F32).astype(BF16)
        if step:
            send(x_own.at[step], x_in.at[me], x_send.at[step], x_recv.at[step], device_at(step))
        else:
            send(x_own.at[0], x_in.at[me], xf_send.at[0], xf_recv.at[0], partner)
            x_in[me] = x_own[0]

    key = jnp.where(first_list >= 0.0, first_list, float(n * rows))
    key_col = column(key)
    rank = jnp.sum(jnp.where((key_col < key) | ((key_col == key) & earlier), 1.0, 0.0), axis=0, keepdims=True)
    rank_col = column(rank)
    first_col = column(first_list)
    sorted_list = jnp.sum(jnp.where(rank_col == iota((slots, slots), 1).astype(F32), first_col, 0.0), axis=0, keepdims=True)
    target_ref[...] = jnp.broadcast_to(jnp.where(sorted_list >= 0.0, sorted_list - low.astype(F32), float(n * rows)).astype(I32), target_ref.shape)
    ids = ids_ref[...]
    all_hots = one_hots(within(ids, chip * CORES * rows, (chip + 1) * CORES * rows), None, DY_ROWS)
    for i in range(n):
        code = (ids[i:i + 1] + 2).astype(F32)
        row_ids = jnp.sum(all_hots[i * DY_ROWS:(i + 1) * DY_ROWS] * code, axis=1, keepdims=True) - 2.0
        picks[i] = jnp.where(row_ids == first_list, 1.0, 0.0).astype(BF16)
        spots[i] = jnp.where(row_ids == sorted_list, 1.0, 0.0).astype(BF16)
    gain32 = wide(g_ref[...])
    x_rows = x_own[...].reshape(slots, hidden)

    def dx_of(block):
        h = jnp.dot(picks[block], x_rows, preferred_element_type=F32)
        r = rms(h)
        xh = h * r
        dy = dy_in[block].astype(F32)
        u = dy * gain32
        dx_all[block] = (r * (u - xh * jnp.mean(u * xh, axis=-1, keepdims=True))).astype(BF16)
        return jnp.sum(dy * xh, axis=0, keepdims=True)

    part = dx_of(me)
    for step in order:
        block = source(step) * CORES + core
        remote(dy_in.at[block], dy_in.at[block], dy_send.at[step], dy_recv.at[step], partner).wait_recv()
        send(dy_in.at[block], dy_in.at[block], dyf_send.at[step], dyf_recv.at[step], partner)
        part = part + dx_of(block)
    for step in [0] + order:
        block = source(step) * CORES + 1 - core
        remote(dy_in.at[block], dy_in.at[block], dyf_send.at[step], dyf_recv.at[step], partner).wait_recv()
        part = part + dx_of(block)
    dg_parts[me] = part
    length = n * DY_ROWS
    sums_ref[...] = lax.dot_general(spots[...].reshape(length, slots), dx_all[...].reshape(length, hidden), TN, preferred_element_type=F32)
    for step in range(1, n):
        send(dg_parts.at[me], dg_parts.at[me], dg_send.at[step], dg_recv.at[step], lax.rem(me + step, n))

    even, odd = ids_ref[pl.ds(chip * CORES, 1)], ids_ref[pl.ds(chip * CORES + 1, 1)]
    here_even, here_odd = even_first[0:1], odd_first[0:1]
    even_mask = jnp.concatenate([within(even, i * rows, (i + 1) * rows) for i in range(n)], axis=0) * here_even
    odd_mask = jnp.concatenate([within(odd, i * rows, (i + 1) * rows) for i in range(n)], axis=0) * here_odd
    pad = jnp.zeros((6, even.shape[1]), F32)
    product = unique_lists(even_mask, odd_mask, jnp.concatenate(halves(even) + (pad,), axis=0), jnp.concatenate(halves(odd) + (pad,), axis=0), X_ROWS)
    held = product[0:1] * 256.0 + product[1:2] - 1.0
    pick = jnp.where(column(my_ids.astype(F32)) == held, 1.0, 0.0).astype(BF16)
    most = jnp.zeros((1, 1), F32)
    for i in range(n):
        count = within(near_even, i * rows, i * rows + rows) * even_first + within(near_odd, i * rows, i * rows + rows) * odd_first
        most = jnp.maximum(most, jnp.max(jnp.sum(count, axis=1, keepdims=True) * (1.0 / X_ROWS), axis=0, keepdims=True))
    for c in range(chips):
        count = jnp.sum(within(ids, c * CORES * rows, (c + 1) * CORES * rows), axis=1, keepdims=True)
        most = jnp.maximum(most, jnp.max(count * (1.0 / DY_ROWS), axis=0, keepdims=True))
    over_ref[0, 0] = jnp.where(most > 1.0005, 1, 0)[0, 0]
    for step in order:
        block = source(step) * CORES + core
        remote(x_in.at[block], x_in.at[block], x_send.at[step], x_recv.at[step], partner).wait_recv()
        send(x_in.at[block], x_in.at[block], xf_send.at[step], xf_recv.at[step], partner)
    for step in range(1, n):
        block = dg_parts.at[lax.rem(me + n - step, n)]
        remote(block, block, dg_send.at[step], dg_recv.at[step], partner).wait_recv()
    total = dg_parts[0]
    for i in range(1, n):
        total = total + dg_parts[i]
    dg_ref[...] = total
    for step in [0] + order:
        block = source(step) * CORES + 1 - core
        remote(x_in.at[block], x_in.at[block], xf_send.at[step], xf_recv.at[step], partner).wait_recv()
    xpos_ref[...] = jnp.dot(pick, x_in[...].reshape(n * X_ROWS, hidden), preferred_element_type=F32).astype(BF16)
    for copy in sent:
        copy.wait_send()


def finish_kernel(zero_rows, target_ref, xpos_ref, sums_ref, g_ref, dg_in, y_ref, de_ref, dg_ref, zeros, targets, zero_sem, row_sem, small_sem):
    blocks = de_ref.shape[0] // zero_rows
    slots = sums_ref.shape[0]
    zeros[...] = jnp.zeros_like(zeros)

    def zero_copy(i):
        return pltpu.make_async_copy(zeros, de_ref.at[pl.ds(pl.multiple_of(i * zero_rows, 8), zero_rows)], zero_sem.at[i])

    for i in range(blocks):
        zero_copy(i).start()
    to_smem = pltpu.make_async_copy(target_ref, targets, small_sem)
    to_smem.start()
    gain = wide(g_ref[...]).astype(BF16)
    h = xpos_ref[...].astype(F32)
    y_ref[...] = (h * rms(h)).astype(BF16) * gain
    for i in range(dg_ref.shape[0]):
        dg_ref[i:i + 1] = dg_in[:, i * 128:(i + 1) * 128]
    to_smem.wait()

    def row_copy(k):
        return pltpu.make_async_copy(sums_ref.at[pl.ds(k, 1)], de_ref.at[pl.ds(targets[0, k], 1)], row_sem)

    def block(i, k):
        zero_copy(i).wait()

        def put(k):
            row_copy(k).start()
            return k + 1
        return lax.while_loop(lambda k: (k < slots) & (targets[0, jnp.minimum(k, slots - 1)] < (i + 1) * zero_rows), put, k)

    count = lax.fori_loop(0, blocks, block, 0)

    def done(k, _):
        row_copy(k).wait()
        return 0

    lax.fori_loop(0, count, done, 0)


def vmem():
    return pl.BlockSpec(memory_space=pltpu.VMEM)


def smem():
    return pl.BlockSpec(memory_space=pltpu.SMEM)


def anywhere():
    return pl.BlockSpec(memory_space=pl.ANY)


def dma(*shape):
    return pltpu.SemaphoreType.DMA(shape)


def pair_exchange_kernel(n, x_out, dy_out, x_in, dy_in, dg_ref, dg_parts, x_send, x_recv, dy_send, dy_recv, dg_send, dg_recv):
    me = lax.axis_index('tp')
    dp = lax.axis_index('dp')
    barrier = pltpu.get_barrier_semaphore()
    for step in range(1, n):
        pl.semaphore_signal(barrier, inc=1, device_id=(dp, lax.rem(me + step, n)), device_id_type=MESH)
    pl.semaphore_wait(barrier, n - 1)

    def copies(src, dst, send_sem, recv_sem, step):
        peer = lax.rem(me + step, n)
        return pltpu.make_async_remote_copy(
            src_ref=src.at[peer], dst_ref=dst.at[me], send_sem=send_sem.at[step], recv_sem=recv_sem.at[step],
            device_id=(dp, peer), device_id_type=MESH)

    def arrival(dst, send_sem, recv_sem, step):
        source = lax.rem(me + n - step, n)
        return pltpu.make_async_remote_copy(
            src_ref=dst.at[source], dst_ref=dst.at[source], send_sem=send_sem.at[step], recv_sem=recv_sem.at[step],
            device_id=(dp, source), device_id_type=MESH)

    x_copies = [copies(x_out, x_in, x_send, x_recv, step) for step in range(1, n)]
    for copy in x_copies:
        copy.start()
    dy_copies = [copies(dy_out, dy_in, dy_send, dy_recv, step) for step in range(1, n)]
    for copy in dy_copies:
        copy.start()
    x_in[me] = x_out[me]
    dy_in[me] = dy_out[me]

    def dg_of(block):
        h = x_in[block].astype(F32)
        return jnp.sum(dy_out[block].astype(F32) * (h * rms(h)), axis=0, keepdims=True)

    for step in range(1, n):
        arrival(x_in, x_send, x_recv, step).wait_recv()
    dg_parts[me] = lax.fori_loop(1, n, lambda i, total: total + dg_of(i), dg_of(0))

    def dg_copy(step):
        return pltpu.make_async_remote_copy(
            src_ref=dg_parts.at[me], dst_ref=dg_parts.at[me], send_sem=dg_send.at[step], recv_sem=dg_recv.at[step],
            device_id=(dp, lax.rem(me + step, n)), device_id_type=MESH)

    dg_copies = [dg_copy(step) for step in range(1, n)]
    for copy in dg_copies:
        copy.start()
    for step in range(1, n):
        arrival(dy_in, dy_send, dy_recv, step).wait_recv()
    for step in range(1, n):
        arrival(dg_parts, dg_send, dg_recv, step).wait_recv()
    for i in range(n):
        dg_ref[i:i + 1] = dg_parts[i]
    for copy in x_copies + dy_copies + dg_copies:
        copy.wait_send()


def any_path(n, ids, table_block, norm_gain, grad_block):
    rows, hidden = table_block.shape
    positions = ids.shape[1]
    cap = positions
    me = lax.axis_index('tp')
    before = (iota((positions, positions), 0) < iota((positions, positions), 1)).astype(I32)

    def slots_of(mask):
        return jnp.sum(mask.astype(I32)[:, :, None] * before[None], axis=1)

    local = ids - me * rows
    mine = (local >= 0) & (local < rows)
    slot = slots_of(mine)
    hit = mine[:, None, :] & (slot[:, None, :] == jnp.arange(cap)[None, :, None])
    wanted = jnp.sum(jnp.where(hit, local[:, None, :] + 1, 0), axis=-1).reshape(n * cap) - 1
    x_own = jnp.take(table_block, jnp.maximum(wanted, 0), axis=0)
    my_ids = lax.dynamic_index_in_dim(ids, me, 0, keepdims=True)
    starts = jnp.arange(n, dtype=I32)[:, None] * rows
    theirs = (my_ids >= starts) & (my_ids < starts + rows)
    their_slot = slots_of(theirs)
    hot = theirs[:, None, :] & (their_slot[:, None, :] == jnp.arange(cap)[None, :, None])
    dy_out = jnp.dot(hot.reshape(n * cap, positions).astype(BF16), grad_block.reshape(positions, hidden))
    slot_of = jnp.sum(jnp.where(theirs, jnp.arange(n)[:, None] * cap + their_slot, 0), axis=0)
    x_in, dy_in, dg = pl.pallas_call(
        functools.partial(pair_exchange_kernel, n),
        out_shape=(jax.ShapeDtypeStruct((n, cap, hidden), BF16), jax.ShapeDtypeStruct((n, cap, hidden), BF16), jax.ShapeDtypeStruct((n, hidden), F32)),
        in_specs=[vmem(), vmem()],
        out_specs=(vmem(), vmem(), vmem()),
        scratch_shapes=[pltpu.VMEM((n, 1, hidden), F32)] + [dma(n)] * 6,
        compiler_params=pltpu.CompilerParams(collective_id=1, has_side_effects=True, vmem_limit_bytes=LIMIT),
        name='exchange_pairs',
    )(x_own.reshape(n, cap, hidden), dy_out.reshape(n, cap, hidden))
    h = jnp.take(x_in.reshape(n * cap, hidden), slot_of, axis=0).astype(F32)
    y = (h * rms(h)).astype(BF16) * norm_gain
    h = x_own.astype(F32)
    r = rms(h)
    xh = h * r
    u = dy_in.reshape(n * cap, hidden).astype(F32) * norm_gain.astype(F32)
    dx = (r * (u - xh * jnp.mean(u * xh, axis=-1, keepdims=True))).astype(BF16)
    grad_table = jax.ops.segment_sum(dx.astype(F32), jnp.where(wanted >= 0, wanted, rows), num_segments=rows)
    return y.reshape(grad_block.shape), grad_table, jnp.sum(dg, axis=0)


def call(kernel, name, out_shape, in_specs, out_specs, scratch_shapes, flops, limit, aliases=None, **params):
    return pl.pallas_call(
        kernel, out_shape=out_shape, in_specs=in_specs, out_specs=out_specs, scratch_shapes=scratch_shapes, name=name,
        input_output_aliases=aliases or {}, cost_estimate=pl.CostEstimate(flops=flops, bytes_accessed=2**24, transcendentals=0),
        compiler_params=pltpu.CompilerParams(vmem_limit_bytes=limit * 2**20, **params))


def device_step(n, token_ids, table_block, norm_gain, grad_block):
    positions = grad_block.shape[0] * grad_block.shape[1]
    rows, hidden = table_block.shape
    ids = token_ids.reshape(n, positions)
    chips = n // CORES
    slots = chips * X_ROWS
    zero_rows = divisor(rows, ZERO_ROWS)
    shape = jax.ShapeDtypeStruct
    gain = norm_gain.reshape(hidden // 128, 128)
    slabs = rows // 8
    xpos, sums, dg, target, over = call(
        functools.partial(exchange_kernel, n, rows), 'exchange',
        (shape((positions, hidden), BF16), shape((slots, hidden), F32), shape((1, hidden), F32), shape((8, slots), I32), shape((1, 1), I32)),
        [vmem(), anywhere(), vmem(), vmem()], (vmem(),) * 4 + (smem(),),
        [pltpu.VMEM((slabs, 8, hidden), BF16), pltpu.VMEM((X_ROWS, 8, hidden), BF16), pltpu.VMEM((8, slots), I32), pltpu.SMEM((8, slots), I32),
         pltpu.VMEM((chips, X_ROWS, hidden), BF16), pltpu.VMEM((n, X_ROWS, hidden), BF16), pltpu.VMEM((chips, DY_ROWS, hidden), BF16),
         pltpu.VMEM((n, DY_ROWS, hidden), BF16), pltpu.VMEM((n, DY_ROWS, slots), BF16), pltpu.VMEM((n, DY_ROWS, slots), BF16),
         pltpu.VMEM((n, DY_ROWS, hidden), BF16), pltpu.VMEM((n, 1, hidden), F32), dma(max(d for d in range(1, 11) if slabs % d == 0)), pltpu.SemaphoreType.DMA]
        + [dma(chips)] * 8 + [dma(n)] * 2, 10**9, 48, collective_id=0, has_side_effects=True)(
            ids, table_block.reshape(slabs, 8, hidden), grad_block.reshape(positions, hidden), gain)
    y, grad_table, dg = call(
        functools.partial(finish_kernel, zero_rows), 'finish',
        (shape((positions, hidden), BF16), shape((rows, hidden), F32), shape((hidden // 128, 128), F32)),
        [anywhere()] + [vmem()] * 4, (vmem(), anywhere(), vmem()),
        [pltpu.VMEM((zero_rows, hidden), F32), pltpu.SMEM((8, slots), I32), dma(rows // zero_rows), pltpu.SemaphoreType.DMA, pltpu.SemaphoreType.DMA],
        10**9, 36)(target, xpos, sums, gain, dg)
    result = y.reshape(grad_block.shape), grad_table, dg.reshape(hidden)

    def general(carry):
        return (jnp.zeros((), I32),) + any_path(n, ids, table_block, norm_gain, grad_block)

    return lax.while_loop(lambda carry: carry[0] > 0, general, (over[0, 0],) + result)[1:]


def solution(mesh):
    return jax.shard_map(functools.partial(device_step, mesh.shape['tp']), mesh=mesh, in_specs=(P('dp', None), P('tp', None), P(None), P('dp', 'tp', None)), out_specs=(P('dp', 'tp', None), P(('dp', 'tp'), None), P('dp')), check_vma=False)
```

```python
import functools

import jax
import jax.numpy as jnp
from jax import lax
from jax.experimental import pallas as pl
from jax.experimental.pallas import tpu as pltpu
from jax.sharding import PartitionSpec as P

RMS_EPS = 1e-5
CORES = 2
X_ROWS = 40
DY_ROWS = 56
ZERO_ROWS = 160
MESH = pl.DeviceIdType.MESH
F32 = jnp.float32
BF16 = jnp.bfloat16
I32 = jnp.int32
NT = (((1,), (1,)), ((), ()))
TN = (((0,), (0,)), ((), ()))
LIMIT = 60 * 2**20


def iota(shape, dim):
    return lax.broadcasted_iota(I32, shape, dim)


def divisor(rows, most):
    return max(d for d in range(8, most + 1, 8) if rows % d == 0)


def rms(h):
    return lax.rsqrt(jnp.mean(h * h, axis=-1, keepdims=True) + RMS_EPS)


def column(row):
    size = row.shape[1]
    return jnp.sum(jnp.where(iota((size, size), 0) == iota((size, size), 1), row, 0.0), axis=1, keepdims=True)


def firsts(even, odd):
    size = even.shape[1]
    before = iota((size, size), 0) < iota((size, size), 1)
    even_col, odd_col = column(even), column(odd)
    even_dup = jnp.where((even_col == even) & before, 1.0, 0.0)
    odd_dup = jnp.where((even_col == odd) | ((odd_col == odd) & before), 1.0, 0.0)
    return 1.0 - jnp.max(even_dup, axis=0, keepdims=True), 1.0 - jnp.max(odd_dup, axis=0, keepdims=True)


def one_hots(mask, offset, cap):
    size = mask.shape[1]
    before = (iota((size, size), 0) < iota((size, size), 1)).astype(BF16)
    rank = jnp.dot(mask.astype(BF16), before, preferred_element_type=F32)
    if offset is not None:
        rank = rank + offset
    rank = jnp.where(mask > 0.0, rank, -1.0).astype(I32)
    slots = iota((cap, size), 0)
    return jnp.concatenate([jnp.where(rank[i:i + 1] == slots, 1.0, 0.0) for i in range(mask.shape[0])], axis=0)


def halves(ids):
    code = ids + 1
    return (code >> 8).astype(F32), (code & 255).astype(F32)


def unique_lists(even_mask, odd_mask, even_code, odd_code, cap):
    even_hot = one_hots(even_mask, None, cap)
    odd_hot = one_hots(odd_mask, jnp.sum(even_mask, axis=1, keepdims=True), cap)
    return (lax.dot_general(even_code.astype(BF16), even_hot.astype(BF16), NT, preferred_element_type=F32)
            + lax.dot_general(odd_code.astype(BF16), odd_hot.astype(BF16), NT, preferred_element_type=F32))


def wide(lines):
    lines = lines.astype(F32)
    return jnp.concatenate([lines[i:i + 1] for i in range(lines.shape[0])], axis=1)


def within(ids, low, high):
    return jnp.where((ids >= low) & (ids < high), 1.0, 0.0)


def exchange_kernel(n, rows, ids_hbm, table_hbm, dy_hbm, g_hbm, xpos_ref, sums_ref, dg_ref, target_ref, over_ref,
                    ids_ref, g_ref, dy_own, table, slabs, local, local_smem, x_own, x_in, dy_out, dy_in, picks, spots, dx_all, dg_parts,
                    table_sem, small_sem, own_sem, x_send, x_recv, xf_send, xf_recv, dy_send, dy_recv, dyf_send, dyf_recv, dg_send, dg_recv):
    chips = n // CORES
    me = lax.axis_index('tp')
    dp = lax.axis_index('dp')
    chip = me // CORES
    core = me % CORES
    partner = chip * CORES + 1 - core
    slots, hidden = sums_ref.shape
    barrier = pltpu.get_barrier_semaphore()
    for step in range(1, n):
        pl.semaphore_signal(barrier, inc=1, device_id=(dp, lax.rem(me + step, n)), device_id_type=MESH)
    load_ids = pltpu.make_async_copy(ids_hbm, ids_ref, own_sem.at[0])
    load_dy = pltpu.make_async_copy(dy_hbm, dy_own, own_sem.at[1])
    load_gain = pltpu.make_async_copy(g_hbm, g_ref, own_sem.at[2])
    for copy in (load_ids, load_dy, load_gain):
        copy.start()
    pieces = table_sem.shape[0]
    piece = table_hbm.shape[0] // pieces
    table_copies = [pltpu.make_async_copy(table_hbm.at[pl.ds(i * piece, piece)], table.at[pl.ds(i * piece, piece)], table_sem.at[i]) for i in range(pieces)]
    def remote(src, dst, send_sem, recv_sem, device):
        return pltpu.make_async_remote_copy(src_ref=src, dst_ref=dst, send_sem=send_sem, recv_sem=recv_sem, device_id=(dp, device), device_id_type=MESH)

    sent = []

    def send(*args):
        copy = remote(*args)
        copy.start()
        sent.append(copy)

    def source(step):
        return lax.rem(chip + chips - step, chips)

    def device_at(step):
        return lax.rem(chip + step, chips) * CORES + core

    order = list(range(2, chips - 1)) + [1, chips - 1]
    low = me * rows

    load_ids.wait()
    my_ids = ids_ref[pl.ds(me, 1)]
    near = [lax.rem(chip + step, chips) for step in range(chips)]
    masks = jnp.concatenate([within(my_ids, c * CORES * rows, (c + 1) * CORES * rows) for c in near], axis=0)
    hots = one_hots(masks, None, DY_ROWS).astype(BF16)
    load_dy.wait()
    load_gain.wait()
    for copy in table_copies:
        copy.start()
    lists = jnp.dot(hots, dy_own[...], preferred_element_type=F32).astype(BF16)
    for step in range(chips):
        dy_out[step] = lists[step * DY_ROWS:(step + 1) * DY_ROWS]
    pl.semaphore_wait(barrier, n - 1)
    for step in order:
        send(dy_out.at[step], dy_in.at[me], dy_send.at[step], dy_recv.at[step], device_at(step))
    send(dy_out.at[0], dy_in.at[me], dyf_send.at[0], dyf_recv.at[0], partner)
    dy_in[me] = dy_out[0]

    even = jnp.concatenate([ids_ref[pl.ds(c * CORES, 1)] for c in near], axis=0)
    odd = jnp.concatenate([ids_ref[pl.ds(c * CORES + 1, 1)] for c in near], axis=0)
    near_even, near_odd = even, odd
    even_f, odd_f = even.astype(F32), odd.astype(F32)
    flags = [firsts(even_f[d:d + 1], odd_f[d:d + 1]) for d in range(chips)]
    even_first = jnp.concatenate([f[0] for f in flags], axis=0)
    odd_first = jnp.concatenate([f[1] for f in flags], axis=0)
    even_code = jnp.concatenate(halves(even), axis=0)
    odd_code = jnp.concatenate(halves(odd), axis=0)
    product = unique_lists(within(even, low, low + rows) * even_first, within(odd, low, low + rows) * odd_first, even_code, odd_code, X_ROWS)
    row_of, slot_of = iota(product.shape, 0), iota(product.shape, 1)
    own_block = (row_of % chips) == (slot_of // X_ROWS)
    wanted = jnp.sum(jnp.where(own_block, product * jnp.where(row_of < chips, 256.0, 1.0), 0.0), axis=0, keepdims=True) - 1.0
    row_in_block = jnp.clip(wanted.astype(I32) - low, 0, rows - 1)
    local[...] = jnp.broadcast_to(row_in_block >> 3, local.shape)
    to_smem = pltpu.make_async_copy(local, local_smem, small_sem)
    to_smem.start()
    remainder = column((row_in_block & 7).astype(F32)).astype(I32)
    wanted_col = column(wanted)
    earlier = iota((slots, slots), 0) < iota((slots, slots), 1)
    repeated = jnp.max(jnp.where((wanted_col == wanted) & earlier, 1.0, 0.0), axis=0, keepdims=True)
    first_list = jnp.where(repeated > 0.0, -1.0, wanted)
    hot_row, hot_col = iota((X_ROWS, X_ROWS * 8), 0), iota((X_ROWS, X_ROWS * 8), 1)
    for copy in table_copies:
        copy.wait()
    to_smem.wait()
    for step in order + [0]:
        def load(s, _, base=step * X_ROWS):
            for j in range(8):
                k = s * 8 + j
                slabs[k] = table[jnp.clip(local_smem[0, base + k], 0, table.shape[0] - 1)]
            return 0
        lax.fori_loop(0, X_ROWS // 8, load, 0)
        pick = jnp.where(hot_col == hot_row * 8 + remainder[step * X_ROWS:(step + 1) * X_ROWS], 1.0, 0.0).astype(BF16)
        x_own[step] = jnp.dot(pick, slabs[...].reshape(X_ROWS * 8, hidden), preferred_element_type=F32).astype(BF16)
        if step:
            send(x_own.at[step], x_in.at[me], x_send.at[step], x_recv.at[step], device_at(step))
        else:
            send(x_own.at[0], x_in.at[me], xf_send.at[0], xf_recv.at[0], partner)
            x_in[me] = x_own[0]

    key = jnp.where(first_list >= 0.0, first_list, float(n * rows))
    key_col = column(key)
    rank = jnp.sum(jnp.where((key_col < key) | ((key_col == key) & earlier), 1.0, 0.0), axis=0, keepdims=True)
    rank_col = column(rank)
    first_col = column(first_list)
    sorted_list = jnp.sum(jnp.where(rank_col == iota((slots, slots), 1).astype(F32), first_col, 0.0), axis=0, keepdims=True)
    target_ref[...] = jnp.broadcast_to(jnp.where(sorted_list >= 0.0, sorted_list - low.astype(F32), float(n * rows)).astype(I32), target_ref.shape)
    ids = ids_ref[...]
    all_hots = one_hots(within(ids, chip * CORES * rows, (chip + 1) * CORES * rows), None, DY_ROWS)
    for i in range(n):
        code = (ids[i:i + 1] + 2).astype(F32)
        row_ids = jnp.sum(all_hots[i * DY_ROWS:(i + 1) * DY_ROWS] * code, axis=1, keepdims=True) - 2.0
        picks[i] = jnp.where(row_ids == first_list, 1.0, 0.0).astype(BF16)
        spots[i] = jnp.where(row_ids == sorted_list, 1.0, 0.0).astype(BF16)
    gain32 = wide(g_ref[...])
    x_rows = x_own[...].reshape(slots, hidden)

    def dx_of(block):
        h = jnp.dot(picks[block], x_rows, preferred_element_type=F32)
        r = rms(h)
        xh = h * r
        dy = dy_in[block].astype(F32)
        u = dy * gain32
        dx_all[block] = (r * (u - xh * jnp.mean(u * xh, axis=-1, keepdims=True))).astype(BF16)
        return jnp.sum(dy * xh, axis=0, keepdims=True)

    part = dx_of(me)
    for step in order:
        block = source(step) * CORES + core
        remote(dy_in.at[block], dy_in.at[block], dy_send.at[step], dy_recv.at[step], partner).wait_recv()
        send(dy_in.at[block], dy_in.at[block], dyf_send.at[step], dyf_recv.at[step], partner)
        part = part + dx_of(block)
    for step in [0] + order:
        block = source(step) * CORES + 1 - core
        remote(dy_in.at[block], dy_in.at[block], dyf_send.at[step], dyf_recv.at[step], partner).wait_recv()
        part = part + dx_of(block)
    dg_parts[me] = part
    length = n * DY_ROWS
    sums_ref[...] = lax.dot_general(spots[...].reshape(length, slots), dx_all[...].reshape(length, hidden), TN, preferred_element_type=F32)
    for step in range(1, n):
        send(dg_parts.at[me], dg_parts.at[me], dg_send.at[step], dg_recv.at[step], lax.rem(me + step, n))

    even, odd = ids_ref[pl.ds(chip * CORES, 1)], ids_ref[pl.ds(chip * CORES + 1, 1)]
    here_even, here_odd = even_first[0:1], odd_first[0:1]
    even_mask = jnp.concatenate([within(even, i * rows, (i + 1) * rows) for i in range(n)], axis=0) * here_even
    odd_mask = jnp.concatenate([within(odd, i * rows, (i + 1) * rows) for i in range(n)], axis=0) * here_odd
    pad = jnp.zeros((6, even.shape[1]), F32)
    product = unique_lists(even_mask, odd_mask, jnp.concatenate(halves(even) + (pad,), axis=0), jnp.concatenate(halves(odd) + (pad,), axis=0), X_ROWS)
    held = product[0:1] * 256.0 + product[1:2] - 1.0
    pick = jnp.where(column(my_ids.astype(F32)) == held, 1.0, 0.0).astype(BF16)
    most = jnp.zeros((1, 1), F32)
    for i in range(n):
        count = within(near_even, i * rows, i * rows + rows) * even_first + within(near_odd, i * rows, i * rows + rows) * odd_first
        most = jnp.maximum(most, jnp.max(jnp.sum(count, axis=1, keepdims=True) * (1.0 / X_ROWS), axis=0, keepdims=True))
    for c in range(chips):
        count = jnp.sum(within(ids, c * CORES * rows, (c + 1) * CORES * rows), axis=1, keepdims=True)
        most = jnp.maximum(most, jnp.max(count * (1.0 / DY_ROWS), axis=0, keepdims=True))
    over_ref[0, 0] = jnp.where(most > 1.0005, 1, 0)[0, 0]
    for step in order:
        block = source(step) * CORES + core
        remote(x_in.at[block], x_in.at[block], x_send.at[step], x_recv.at[step], partner).wait_recv()
        send(x_in.at[block], x_in.at[block], xf_send.at[step], xf_recv.at[step], partner)
    for step in range(1, n):
        block = dg_parts.at[lax.rem(me + n - step, n)]
        remote(block, block, dg_send.at[step], dg_recv.at[step], partner).wait_recv()
    total = dg_parts[0]
    for i in range(1, n):
        total = total + dg_parts[i]
    dg_ref[...] = total
    for step in [0] + order:
        block = source(step) * CORES + 1 - core
        remote(x_in.at[block], x_in.at[block], xf_send.at[step], xf_recv.at[step], partner).wait_recv()
    xpos_ref[...] = jnp.dot(pick, x_in[...].reshape(n * X_ROWS, hidden), preferred_element_type=F32).astype(BF16)
    for copy in sent:
        copy.wait_send()


def finish_kernel(zero_rows, target_ref, xpos_ref, sums_ref, g_ref, dg_in, y_hbm, de_ref, dg_hbm, zeros, targets, y_ref, dg_ref, zero_sem, row_sem, small_sem, out_sem):
    blocks = de_ref.shape[0] // zero_rows
    slots = sums_ref.shape[0]
    zeros[...] = jnp.zeros_like(zeros)

    def zero_copy(i):
        return pltpu.make_async_copy(zeros, de_ref.at[pl.ds(pl.multiple_of(i * zero_rows, 8), zero_rows)], zero_sem.at[i])

    for i in range(blocks):
        zero_copy(i).start()
    to_smem = pltpu.make_async_copy(target_ref, targets, small_sem)
    to_smem.start()
    gain = wide(g_ref[...]).astype(BF16)
    h = xpos_ref[...].astype(F32)
    y_ref[...] = (h * rms(h)).astype(BF16) * gain
    for i in range(dg_ref.shape[0]):
        dg_ref[i:i + 1] = dg_in[:, i * 128:(i + 1) * 128]
    outs = [pltpu.make_async_copy(y_ref, y_hbm, out_sem.at[0]), pltpu.make_async_copy(dg_ref, dg_hbm, out_sem.at[1])]
    for copy in outs:
        copy.start()
    to_smem.wait()

    def row_copy(k):
        return pltpu.make_async_copy(sums_ref.at[pl.ds(k, 1)], de_ref.at[pl.ds(targets[0, k], 1)], row_sem)

    def block(i, k):
        zero_copy(i).wait()

        def put(k):
            row_copy(k).start()
            return k + 1
        return lax.while_loop(lambda k: (k < slots) & (targets[0, jnp.minimum(k, slots - 1)] < (i + 1) * zero_rows), put, k)

    count = lax.fori_loop(0, blocks, block, 0)

    def done(k, _):
        row_copy(k).wait()
        return 0

    lax.fori_loop(0, count, done, 0)
    for copy in outs:
        copy.wait()


def vmem():
    return pl.BlockSpec(memory_space=pltpu.VMEM)


def smem():
    return pl.BlockSpec(memory_space=pltpu.SMEM)


def anywhere():
    return pl.BlockSpec(memory_space=pl.ANY)


def dma(*shape):
    return pltpu.SemaphoreType.DMA(shape)


def pair_exchange_kernel(n, x_out, dy_out, x_in, dy_in, dg_ref, dg_parts, x_send, x_recv, dy_send, dy_recv, dg_send, dg_recv):
    me = lax.axis_index('tp')
    dp = lax.axis_index('dp')
    barrier = pltpu.get_barrier_semaphore()
    for step in range(1, n):
        pl.semaphore_signal(barrier, inc=1, device_id=(dp, lax.rem(me + step, n)), device_id_type=MESH)
    pl.semaphore_wait(barrier, n - 1)

    def copies(src, dst, send_sem, recv_sem, step):
        peer = lax.rem(me + step, n)
        return pltpu.make_async_remote_copy(
            src_ref=src.at[peer], dst_ref=dst.at[me], send_sem=send_sem.at[step], recv_sem=recv_sem.at[step],
            device_id=(dp, peer), device_id_type=MESH)

    def arrival(dst, send_sem, recv_sem, step):
        source = lax.rem(me + n - step, n)
        return pltpu.make_async_remote_copy(
            src_ref=dst.at[source], dst_ref=dst.at[source], send_sem=send_sem.at[step], recv_sem=recv_sem.at[step],
            device_id=(dp, source), device_id_type=MESH)

    x_copies = [copies(x_out, x_in, x_send, x_recv, step) for step in range(1, n)]
    for copy in x_copies:
        copy.start()
    dy_copies = [copies(dy_out, dy_in, dy_send, dy_recv, step) for step in range(1, n)]
    for copy in dy_copies:
        copy.start()
    x_in[me] = x_out[me]
    dy_in[me] = dy_out[me]

    def dg_of(block):
        h = x_in[block].astype(F32)
        return jnp.sum(dy_out[block].astype(F32) * (h * rms(h)), axis=0, keepdims=True)

    for step in range(1, n):
        arrival(x_in, x_send, x_recv, step).wait_recv()
    dg_parts[me] = lax.fori_loop(1, n, lambda i, total: total + dg_of(i), dg_of(0))

    def dg_copy(step):
        return pltpu.make_async_remote_copy(
            src_ref=dg_parts.at[me], dst_ref=dg_parts.at[me], send_sem=dg_send.at[step], recv_sem=dg_recv.at[step],
            device_id=(dp, lax.rem(me + step, n)), device_id_type=MESH)

    dg_copies = [dg_copy(step) for step in range(1, n)]
    for copy in dg_copies:
        copy.start()
    for step in range(1, n):
        arrival(dy_in, dy_send, dy_recv, step).wait_recv()
    for step in range(1, n):
        arrival(dg_parts, dg_send, dg_recv, step).wait_recv()
    for i in range(n):
        dg_ref[i:i + 1] = dg_parts[i]
    for copy in x_copies + dy_copies + dg_copies:
        copy.wait_send()


def any_path(n, ids, table_block, norm_gain, grad_block):
    rows, hidden = table_block.shape
    positions = ids.shape[1]
    cap = positions
    me = lax.axis_index('tp')
    before = (iota((positions, positions), 0) < iota((positions, positions), 1)).astype(I32)

    def slots_of(mask):
        return jnp.sum(mask.astype(I32)[:, :, None] * before[None], axis=1)

    local = ids - me * rows
    mine = (local >= 0) & (local < rows)
    slot = slots_of(mine)
    hit = mine[:, None, :] & (slot[:, None, :] == jnp.arange(cap)[None, :, None])
    wanted = jnp.sum(jnp.where(hit, local[:, None, :] + 1, 0), axis=-1).reshape(n * cap) - 1
    x_own = jnp.take(table_block, jnp.maximum(wanted, 0), axis=0)
    my_ids = lax.dynamic_index_in_dim(ids, me, 0, keepdims=True)
    starts = jnp.arange(n, dtype=I32)[:, None] * rows
    theirs = (my_ids >= starts) & (my_ids < starts + rows)
    their_slot = slots_of(theirs)
    hot = theirs[:, None, :] & (their_slot[:, None, :] == jnp.arange(cap)[None, :, None])
    dy_out = jnp.dot(hot.reshape(n * cap, positions).astype(BF16), grad_block.reshape(positions, hidden))
    slot_of = jnp.sum(jnp.where(theirs, jnp.arange(n)[:, None] * cap + their_slot, 0), axis=0)
    x_in, dy_in, dg = pl.pallas_call(
        functools.partial(pair_exchange_kernel, n),
        out_shape=(jax.ShapeDtypeStruct((n, cap, hidden), BF16), jax.ShapeDtypeStruct((n, cap, hidden), BF16), jax.ShapeDtypeStruct((n, hidden), F32)),
        in_specs=[vmem(), vmem()],
        out_specs=(vmem(), vmem(), vmem()),
        scratch_shapes=[pltpu.VMEM((n, 1, hidden), F32)] + [dma(n)] * 6,
        compiler_params=pltpu.CompilerParams(collective_id=1, has_side_effects=True, vmem_limit_bytes=LIMIT),
        name='exchange_pairs',
    )(x_own.reshape(n, cap, hidden), dy_out.reshape(n, cap, hidden))
    h = jnp.take(x_in.reshape(n * cap, hidden), slot_of, axis=0).astype(F32)
    y = (h * rms(h)).astype(BF16) * norm_gain
    h = x_own.astype(F32)
    r = rms(h)
    xh = h * r
    u = dy_in.reshape(n * cap, hidden).astype(F32) * norm_gain.astype(F32)
    dx = (r * (u - xh * jnp.mean(u * xh, axis=-1, keepdims=True))).astype(BF16)
    grad_table = jax.ops.segment_sum(dx.astype(F32), jnp.where(wanted >= 0, wanted, rows), num_segments=rows)
    return y.reshape(grad_block.shape), grad_table, jnp.sum(dg, axis=0)


def call(kernel, name, out_shape, in_specs, out_specs, scratch_shapes, flops, limit, aliases=None, **params):
    return pl.pallas_call(
        kernel, out_shape=out_shape, in_specs=in_specs, out_specs=out_specs, scratch_shapes=scratch_shapes, name=name,
        input_output_aliases=aliases or {}, cost_estimate=pl.CostEstimate(flops=flops, bytes_accessed=2**24, transcendentals=0),
        compiler_params=pltpu.CompilerParams(vmem_limit_bytes=limit * 2**20, **params))


def device_step(n, token_ids, table_block, norm_gain, grad_block):
    positions = grad_block.shape[0] * grad_block.shape[1]
    rows, hidden = table_block.shape
    ids = token_ids.reshape(n, positions)
    chips = n // CORES
    slots = chips * X_ROWS
    zero_rows = divisor(rows, ZERO_ROWS)
    shape = jax.ShapeDtypeStruct
    gain = norm_gain.reshape(hidden // 128, 128)
    slabs = rows // 8
    xpos, sums, dg, target, over = call(
        functools.partial(exchange_kernel, n, rows), 'exchange',
        (shape((positions, hidden), BF16), shape((slots, hidden), F32), shape((1, hidden), F32), shape((8, slots), I32), shape((1, 1), I32)),
        [anywhere()] * 4, (vmem(),) * 4 + (smem(),),
        [pltpu.VMEM((n, positions), I32), pltpu.VMEM((hidden // 128, 128), BF16), pltpu.VMEM((positions, hidden), BF16), pltpu.VMEM((slabs, 8, hidden), BF16), pltpu.VMEM((X_ROWS, 8, hidden), BF16), pltpu.VMEM((8, slots), I32), pltpu.SMEM((8, slots), I32),
         pltpu.VMEM((chips, X_ROWS, hidden), BF16), pltpu.VMEM((n, X_ROWS, hidden), BF16), pltpu.VMEM((chips, DY_ROWS, hidden), BF16),
         pltpu.VMEM((n, DY_ROWS, hidden), BF16), pltpu.VMEM((n, DY_ROWS, slots), BF16), pltpu.VMEM((n, DY_ROWS, slots), BF16),
         pltpu.VMEM((n, DY_ROWS, hidden), BF16), pltpu.VMEM((n, 1, hidden), F32), dma(max(d for d in range(1, 11) if slabs % d == 0)), pltpu.SemaphoreType.DMA, dma(3)]
        + [dma(chips)] * 8 + [dma(n)] * 2, 10**9, 48, collective_id=0, has_side_effects=True)(
            ids, table_block.reshape(slabs, 8, hidden), grad_block.reshape(positions, hidden), gain)
    y, grad_table, dg = call(
        functools.partial(finish_kernel, zero_rows), 'finish',
        (shape((positions, hidden), BF16), shape((rows, hidden), F32), shape((hidden // 128, 128), F32)),
        [anywhere()] + [vmem()] * 4, (anywhere(),) * 3,
        [pltpu.VMEM((zero_rows, hidden), F32), pltpu.SMEM((8, slots), I32), pltpu.VMEM((positions, hidden), BF16), pltpu.VMEM((hidden // 128, 128), F32),
         dma(rows // zero_rows), pltpu.SemaphoreType.DMA, pltpu.SemaphoreType.DMA, dma(2)],
        10**9, 36)(target, xpos, sums, gain, dg)
    result = y.reshape(grad_block.shape), grad_table, dg.reshape(hidden)

    def general(carry):
        return (jnp.zeros((), I32),) + any_path(n, ids, table_block, norm_gain, grad_block)

    return lax.while_loop(lambda carry: carry[0] > 0, general, (over[0, 0],) + result)[1:]


def solution(mesh):
    return jax.shard_map(functools.partial(device_step, mesh.shape['tp']), mesh=mesh, in_specs=(P('dp', None), P('tp', None), P(None), P('dp', 'tp', None)), out_specs=(P('dp', 'tp', None), P(('dp', 'tp'), None), P('dp')), check_vma=False)
```

```python
import functools

import jax
import jax.numpy as jnp
from jax import lax
from jax.experimental import pallas as pl
from jax.experimental.pallas import tpu as pltpu
from jax.sharding import PartitionSpec as P

RMS_EPS = 1e-5
CORES = 2
X_ROWS = 40
DY_ROWS = 56
ZERO_ROWS = 160
MESH = pl.DeviceIdType.MESH
F32 = jnp.float32
BF16 = jnp.bfloat16
I32 = jnp.int32
NT = (((1,), (1,)), ((), ()))
TN = (((0,), (0,)), ((), ()))
LIMIT = 60 * 2**20


def iota(shape, dim):
    return lax.broadcasted_iota(I32, shape, dim)


def divisor(rows, most):
    return max(d for d in range(8, most + 1, 8) if rows % d == 0)


def rms(h):
    return lax.rsqrt(jnp.mean(h * h, axis=-1, keepdims=True) + RMS_EPS)


def column(row):
    size = row.shape[1]
    return jnp.sum(jnp.where(iota((size, size), 0) == iota((size, size), 1), row, 0.0), axis=1, keepdims=True)


def firsts(even, odd):
    size = even.shape[1]
    before = iota((size, size), 0) < iota((size, size), 1)
    even_col, odd_col = column(even), column(odd)
    even_dup = jnp.where((even_col == even) & before, 1.0, 0.0)
    odd_dup = jnp.where((even_col == odd) | ((odd_col == odd) & before), 1.0, 0.0)
    return 1.0 - jnp.max(even_dup, axis=0, keepdims=True), 1.0 - jnp.max(odd_dup, axis=0, keepdims=True)


def one_hots(mask, offset, cap):
    size = mask.shape[1]
    before = (iota((size, size), 0) < iota((size, size), 1)).astype(BF16)
    rank = jnp.dot(mask.astype(BF16), before, preferred_element_type=F32)
    if offset is not None:
        rank = rank + offset
    rank = jnp.where(mask > 0.0, rank, -1.0).astype(I32)
    slots = iota((cap, size), 0)
    return jnp.concatenate([jnp.where(rank[i:i + 1] == slots, 1.0, 0.0) for i in range(mask.shape[0])], axis=0)


def halves(ids):
    code = ids + 1
    return (code >> 8).astype(F32), (code & 255).astype(F32)


def unique_lists(even_mask, odd_mask, even_code, odd_code, cap):
    even_hot = one_hots(even_mask, None, cap)
    odd_hot = one_hots(odd_mask, jnp.sum(even_mask, axis=1, keepdims=True), cap)
    return (lax.dot_general(even_code.astype(BF16), even_hot.astype(BF16), NT, preferred_element_type=F32)
            + lax.dot_general(odd_code.astype(BF16), odd_hot.astype(BF16), NT, preferred_element_type=F32))


def wide(lines):
    lines = lines.astype(F32)
    return jnp.concatenate([lines[i:i + 1] for i in range(lines.shape[0])], axis=1)


def within(ids, low, high):
    return jnp.where((ids >= low) & (ids < high), 1.0, 0.0)


def exchange_kernel(n, rows, ids_hbm, table_hbm, dy_hbm, g_hbm, xpos_ref, sums_ref, dg_ref, target_ref, over_hbm,
                    over_ref, ids_ref, g_ref, dy_own, table, slabs, local, local_smem, x_own, x_in, dy_out, dy_in, picks, spots, dx_all, dg_parts,
                    table_sem, small_sem, own_sem, x_send, x_recv, xf_send, xf_recv, dy_send, dy_recv, dyf_send, dyf_recv, dg_send, dg_recv):
    chips = n // CORES
    me = lax.axis_index('tp')
    dp = lax.axis_index('dp')
    chip = me // CORES
    core = me % CORES
    partner = chip * CORES + 1 - core
    slots, hidden = sums_ref.shape
    barrier = pltpu.get_barrier_semaphore()
    for step in range(1, n):
        pl.semaphore_signal(barrier, inc=1, device_id=(dp, lax.rem(me + step, n)), device_id_type=MESH)
    load_ids = pltpu.make_async_copy(ids_hbm, ids_ref, own_sem.at[0])
    load_dy = pltpu.make_async_copy(dy_hbm, dy_own, own_sem.at[1])
    load_gain = pltpu.make_async_copy(g_hbm, g_ref, own_sem.at[2])
    for copy in (load_ids, load_dy, load_gain):
        copy.start()
    pieces = table_sem.shape[0]
    piece = table_hbm.shape[0] // pieces
    table_copies = [pltpu.make_async_copy(table_hbm.at[pl.ds(i * piece, piece)], table.at[pl.ds(i * piece, piece)], table_sem.at[i]) for i in range(pieces)]
    def remote(src, dst, send_sem, recv_sem, device):
        return pltpu.make_async_remote_copy(src_ref=src, dst_ref=dst, send_sem=send_sem, recv_sem=recv_sem, device_id=(dp, device), device_id_type=MESH)

    sent = []

    def send(*args):
        copy = remote(*args)
        copy.start()
        sent.append(copy)

    def source(step):
        return lax.rem(chip + chips - step, chips)

    def device_at(step):
        return lax.rem(chip + step, chips) * CORES + core

    order = list(range(2, chips - 1)) + [1, chips - 1]
    low = me * rows

    load_ids.wait()
    my_ids = ids_ref[pl.ds(me, 1)]
    near = [lax.rem(chip + step, chips) for step in range(chips)]
    masks = jnp.concatenate([within(my_ids, c * CORES * rows, (c + 1) * CORES * rows) for c in near], axis=0)
    hots = one_hots(masks, None, DY_ROWS).astype(BF16)
    load_dy.wait()
    load_gain.wait()
    for copy in table_copies:
        copy.start()
    lists = jnp.dot(hots, dy_own[...], preferred_element_type=F32).astype(BF16)
    for step in range(chips):
        dy_out[step] = lists[step * DY_ROWS:(step + 1) * DY_ROWS]
    pl.semaphore_wait(barrier, n - 1)
    for step in order:
        send(dy_out.at[step], dy_in.at[me], dy_send.at[step], dy_recv.at[step], device_at(step))
    send(dy_out.at[0], dy_in.at[me], dyf_send.at[0], dyf_recv.at[0], partner)
    dy_in[me] = dy_out[0]

    even = jnp.concatenate([ids_ref[pl.ds(c * CORES, 1)] for c in near], axis=0)
    odd = jnp.concatenate([ids_ref[pl.ds(c * CORES + 1, 1)] for c in near], axis=0)
    near_even, near_odd = even, odd
    even_f, odd_f = even.astype(F32), odd.astype(F32)
    flags = [firsts(even_f[d:d + 1], odd_f[d:d + 1]) for d in range(chips)]
    even_first = jnp.concatenate([f[0] for f in flags], axis=0)
    odd_first = jnp.concatenate([f[1] for f in flags], axis=0)
    even_code = jnp.concatenate(halves(even), axis=0)
    odd_code = jnp.concatenate(halves(odd), axis=0)
    product = unique_lists(within(even, low, low + rows) * even_first, within(odd, low, low + rows) * odd_first, even_code, odd_code, X_ROWS)
    row_of, slot_of = iota(product.shape, 0), iota(product.shape, 1)
    own_block = (row_of % chips) == (slot_of // X_ROWS)
    wanted = jnp.sum(jnp.where(own_block, product * jnp.where(row_of < chips, 256.0, 1.0), 0.0), axis=0, keepdims=True) - 1.0
    row_in_block = jnp.clip(wanted.astype(I32) - low, 0, rows - 1)
    local[...] = jnp.broadcast_to(row_in_block >> 3, local.shape)
    to_smem = pltpu.make_async_copy(local, local_smem, small_sem)
    to_smem.start()
    remainder = column((row_in_block & 7).astype(F32)).astype(I32)
    wanted_col = column(wanted)
    earlier = iota((slots, slots), 0) < iota((slots, slots), 1)
    repeated = jnp.max(jnp.where((wanted_col == wanted) & earlier, 1.0, 0.0), axis=0, keepdims=True)
    first_list = jnp.where(repeated > 0.0, -1.0, wanted)
    hot_row, hot_col = iota((X_ROWS, X_ROWS * 8), 0), iota((X_ROWS, X_ROWS * 8), 1)
    for copy in table_copies:
        copy.wait()
    to_smem.wait()
    for step in order + [0]:
        def load(s, _, base=step * X_ROWS):
            for j in range(8):
                k = s * 8 + j
                slabs[k] = table[jnp.clip(local_smem[0, base + k], 0, table.shape[0] - 1)]
            return 0
        lax.fori_loop(0, X_ROWS // 8, load, 0)
        pick = jnp.where(hot_col == hot_row * 8 + remainder[step * X_ROWS:(step + 1) * X_ROWS], 1.0, 0.0).astype(BF16)
        x_own[step] = jnp.dot(pick, slabs[...].reshape(X_ROWS * 8, hidden), preferred_element_type=F32).astype(BF16)
        if step:
            send(x_own.at[step], x_in.at[me], x_send.at[step], x_recv.at[step], device_at(step))
        else:
            send(x_own.at[0], x_in.at[me], xf_send.at[0], xf_recv.at[0], partner)
            x_in[me] = x_own[0]

    key = jnp.where(first_list >= 0.0, first_list, float(n * rows))
    key_col = column(key)
    rank = jnp.sum(jnp.where((key_col < key) | ((key_col == key) & earlier), 1.0, 0.0), axis=0, keepdims=True)
    rank_col = column(rank)
    first_col = column(first_list)
    sorted_list = jnp.sum(jnp.where(rank_col == iota((slots, slots), 1).astype(F32), first_col, 0.0), axis=0, keepdims=True)
    target_ref[...] = jnp.broadcast_to(jnp.where(sorted_list >= 0.0, sorted_list - low.astype(F32), float(n * rows)).astype(I32), target_ref.shape)
    ids = ids_ref[...]
    all_hots = one_hots(within(ids, chip * CORES * rows, (chip + 1) * CORES * rows), None, DY_ROWS)
    for i in range(n):
        code = (ids[i:i + 1] + 2).astype(F32)
        row_ids = jnp.sum(all_hots[i * DY_ROWS:(i + 1) * DY_ROWS] * code, axis=1, keepdims=True) - 2.0
        picks[i] = jnp.where(row_ids == first_list, 1.0, 0.0).astype(BF16)
        spots[i] = jnp.where(row_ids == sorted_list, 1.0, 0.0).astype(BF16)
    gain32 = wide(g_ref[...])
    x_rows = x_own[...].reshape(slots, hidden)

    def dx_of(block):
        h = jnp.dot(picks[block], x_rows, preferred_element_type=F32)
        r = rms(h)
        xh = h * r
        dy = dy_in[block].astype(F32)
        u = dy * gain32
        dx_all[block] = (r * (u - xh * jnp.mean(u * xh, axis=-1, keepdims=True))).astype(BF16)
        return jnp.sum(dy * xh, axis=0, keepdims=True)

    part = dx_of(me)
    for step in order:
        block = source(step) * CORES + core
        remote(dy_in.at[block], dy_in.at[block], dy_send.at[step], dy_recv.at[step], partner).wait_recv()
        send(dy_in.at[block], dy_in.at[block], dyf_send.at[step], dyf_recv.at[step], partner)
        part = part + dx_of(block)
    for step in [0] + order:
        block = source(step) * CORES + 1 - core
        remote(dy_in.at[block], dy_in.at[block], dyf_send.at[step], dyf_recv.at[step], partner).wait_recv()
        part = part + dx_of(block)
    dg_parts[me] = part
    length = n * DY_ROWS
    sums_ref[...] = lax.dot_general(spots[...].reshape(length, slots), dx_all[...].reshape(length, hidden), TN, preferred_element_type=F32)
    for step in range(1, n):
        send(dg_parts.at[me], dg_parts.at[me], dg_send.at[step], dg_recv.at[step], lax.rem(me + step, n))

    even, odd = ids_ref[pl.ds(chip * CORES, 1)], ids_ref[pl.ds(chip * CORES + 1, 1)]
    here_even, here_odd = even_first[0:1], odd_first[0:1]
    even_mask = jnp.concatenate([within(even, i * rows, (i + 1) * rows) for i in range(n)], axis=0) * here_even
    odd_mask = jnp.concatenate([within(odd, i * rows, (i + 1) * rows) for i in range(n)], axis=0) * here_odd
    pad = jnp.zeros((6, even.shape[1]), F32)
    product = unique_lists(even_mask, odd_mask, jnp.concatenate(halves(even) + (pad,), axis=0), jnp.concatenate(halves(odd) + (pad,), axis=0), X_ROWS)
    held = product[0:1] * 256.0 + product[1:2] - 1.0
    pick = jnp.where(column(my_ids.astype(F32)) == held, 1.0, 0.0).astype(BF16)
    most = jnp.zeros((1, 1), F32)
    for i in range(n):
        count = within(near_even, i * rows, i * rows + rows) * even_first + within(near_odd, i * rows, i * rows + rows) * odd_first
        most = jnp.maximum(most, jnp.max(jnp.sum(count, axis=1, keepdims=True) * (1.0 / X_ROWS), axis=0, keepdims=True))
    for c in range(chips):
        count = jnp.sum(within(ids, c * CORES * rows, (c + 1) * CORES * rows), axis=1, keepdims=True)
        most = jnp.maximum(most, jnp.max(count * (1.0 / DY_ROWS), axis=0, keepdims=True))
    over_ref[0, 0] = jnp.where(most > 1.0005, 1, 0)[0, 0]
    put_over = pltpu.make_async_copy(over_ref, over_hbm, own_sem.at[0])
    put_over.start()
    for step in order:
        block = source(step) * CORES + core
        remote(x_in.at[block], x_in.at[block], x_send.at[step], x_recv.at[step], partner).wait_recv()
        send(x_in.at[block], x_in.at[block], xf_send.at[step], xf_recv.at[step], partner)
    for step in range(1, n):
        block = dg_parts.at[lax.rem(me + n - step, n)]
        remote(block, block, dg_send.at[step], dg_recv.at[step], partner).wait_recv()
    total = dg_parts[0]
    for i in range(1, n):
        total = total + dg_parts[i]
    dg_ref[...] = total
    for step in [0] + order:
        block = source(step) * CORES + 1 - core
        remote(x_in.at[block], x_in.at[block], xf_send.at[step], xf_recv.at[step], partner).wait_recv()
    xpos_ref[...] = jnp.dot(pick, x_in[...].reshape(n * X_ROWS, hidden), preferred_element_type=F32).astype(BF16)
    for copy in sent:
        copy.wait_send()
    put_over.wait()


def finish_kernel(zero_rows, target_ref, xpos_ref, sums_ref, g_ref, dg_in, y_hbm, de_ref, dg_hbm, zeros, targets, y_ref, dg_ref, zero_sem, row_sem, small_sem, out_sem):
    blocks = de_ref.shape[0] // zero_rows
    slots = sums_ref.shape[0]
    zeros[...] = jnp.zeros_like(zeros)

    def zero_copy(i):
        return pltpu.make_async_copy(zeros, de_ref.at[pl.ds(pl.multiple_of(i * zero_rows, 8), zero_rows)], zero_sem.at[i])

    for i in range(blocks):
        zero_copy(i).start()
    to_smem = pltpu.make_async_copy(target_ref, targets, small_sem)
    to_smem.start()
    gain = wide(g_ref[...]).astype(BF16)
    h = xpos_ref[...].astype(F32)
    y_ref[...] = (h * rms(h)).astype(BF16) * gain
    for i in range(dg_ref.shape[0]):
        dg_ref[i:i + 1] = dg_in[:, i * 128:(i + 1) * 128]
    outs = [pltpu.make_async_copy(y_ref, y_hbm, out_sem.at[0]), pltpu.make_async_copy(dg_ref, dg_hbm, out_sem.at[1])]
    for copy in outs:
        copy.start()
    to_smem.wait()

    def row_copy(k):
        return pltpu.make_async_copy(sums_ref.at[pl.ds(k, 1)], de_ref.at[pl.ds(targets[0, k], 1)], row_sem)

    def block(i, k):
        zero_copy(i).wait()

        def put(k):
            row_copy(k).start()
            return k + 1
        return lax.while_loop(lambda k: (k < slots) & (targets[0, jnp.minimum(k, slots - 1)] < (i + 1) * zero_rows), put, k)

    count = lax.fori_loop(0, blocks, block, 0)

    def done(k, _):
        row_copy(k).wait()
        return 0

    lax.fori_loop(0, count, done, 0)
    for copy in outs:
        copy.wait()


def vmem():
    return pl.BlockSpec(memory_space=pltpu.VMEM)


def smem():
    return pl.BlockSpec(memory_space=pltpu.SMEM)


def anywhere():
    return pl.BlockSpec(memory_space=pl.ANY)


def dma(*shape):
    return pltpu.SemaphoreType.DMA(shape)


def pair_exchange_kernel(n, x_out, dy_out, x_in, dy_in, dg_ref, dg_parts, x_send, x_recv, dy_send, dy_recv, dg_send, dg_recv):
    me = lax.axis_index('tp')
    dp = lax.axis_index('dp')
    barrier = pltpu.get_barrier_semaphore()
    for step in range(1, n):
        pl.semaphore_signal(barrier, inc=1, device_id=(dp, lax.rem(me + step, n)), device_id_type=MESH)
    pl.semaphore_wait(barrier, n - 1)

    def copies(src, dst, send_sem, recv_sem, step):
        peer = lax.rem(me + step, n)
        return pltpu.make_async_remote_copy(
            src_ref=src.at[peer], dst_ref=dst.at[me], send_sem=send_sem.at[step], recv_sem=recv_sem.at[step],
            device_id=(dp, peer), device_id_type=MESH)

    def arrival(dst, send_sem, recv_sem, step):
        source = lax.rem(me + n - step, n)
        return pltpu.make_async_remote_copy(
            src_ref=dst.at[source], dst_ref=dst.at[source], send_sem=send_sem.at[step], recv_sem=recv_sem.at[step],
            device_id=(dp, source), device_id_type=MESH)

    x_copies = [copies(x_out, x_in, x_send, x_recv, step) for step in range(1, n)]
    for copy in x_copies:
        copy.start()
    dy_copies = [copies(dy_out, dy_in, dy_send, dy_recv, step) for step in range(1, n)]
    for copy in dy_copies:
        copy.start()
    x_in[me] = x_out[me]
    dy_in[me] = dy_out[me]

    def dg_of(block):
        h = x_in[block].astype(F32)
        return jnp.sum(dy_out[block].astype(F32) * (h * rms(h)), axis=0, keepdims=True)

    for step in range(1, n):
        arrival(x_in, x_send, x_recv, step).wait_recv()
    dg_parts[me] = lax.fori_loop(1, n, lambda i, total: total + dg_of(i), dg_of(0))

    def dg_copy(step):
        return pltpu.make_async_remote_copy(
            src_ref=dg_parts.at[me], dst_ref=dg_parts.at[me], send_sem=dg_send.at[step], recv_sem=dg_recv.at[step],
            device_id=(dp, lax.rem(me + step, n)), device_id_type=MESH)

    dg_copies = [dg_copy(step) for step in range(1, n)]
    for copy in dg_copies:
        copy.start()
    for step in range(1, n):
        arrival(dy_in, dy_send, dy_recv, step).wait_recv()
    for step in range(1, n):
        arrival(dg_parts, dg_send, dg_recv, step).wait_recv()
    for i in range(n):
        dg_ref[i:i + 1] = dg_parts[i]
    for copy in x_copies + dy_copies + dg_copies:
        copy.wait_send()


def any_path(n, ids, table_block, norm_gain, grad_block):
    rows, hidden = table_block.shape
    positions = ids.shape[1]
    cap = positions
    me = lax.axis_index('tp')
    before = (iota((positions, positions), 0) < iota((positions, positions), 1)).astype(I32)

    def slots_of(mask):
        return jnp.sum(mask.astype(I32)[:, :, None] * before[None], axis=1)

    local = ids - me * rows
    mine = (local >= 0) & (local < rows)
    slot = slots_of(mine)
    hit = mine[:, None, :] & (slot[:, None, :] == jnp.arange(cap)[None, :, None])
    wanted = jnp.sum(jnp.where(hit, local[:, None, :] + 1, 0), axis=-1).reshape(n * cap) - 1
    x_own = jnp.take(table_block, jnp.maximum(wanted, 0), axis=0)
    my_ids = lax.dynamic_index_in_dim(ids, me, 0, keepdims=True)
    starts = jnp.arange(n, dtype=I32)[:, None] * rows
    theirs = (my_ids >= starts) & (my_ids < starts + rows)
    their_slot = slots_of(theirs)
    hot = theirs[:, None, :] & (their_slot[:, None, :] == jnp.arange(cap)[None, :, None])
    dy_out = jnp.dot(hot.reshape(n * cap, positions).astype(BF16), grad_block.reshape(positions, hidden))
    slot_of = jnp.sum(jnp.where(theirs, jnp.arange(n)[:, None] * cap + their_slot, 0), axis=0)
    x_in, dy_in, dg = pl.pallas_call(
        functools.partial(pair_exchange_kernel, n),
        out_shape=(jax.ShapeDtypeStruct((n, cap, hidden), BF16), jax.ShapeDtypeStruct((n, cap, hidden), BF16), jax.ShapeDtypeStruct((n, hidden), F32)),
        in_specs=[vmem(), vmem()],
        out_specs=(vmem(), vmem(), vmem()),
        scratch_shapes=[pltpu.VMEM((n, 1, hidden), F32)] + [dma(n)] * 6,
        compiler_params=pltpu.CompilerParams(collective_id=1, has_side_effects=True, vmem_limit_bytes=LIMIT),
        name='exchange_pairs',
    )(x_own.reshape(n, cap, hidden), dy_out.reshape(n, cap, hidden))
    h = jnp.take(x_in.reshape(n * cap, hidden), slot_of, axis=0).astype(F32)
    y = (h * rms(h)).astype(BF16) * norm_gain
    h = x_own.astype(F32)
    r = rms(h)
    xh = h * r
    u = dy_in.reshape(n * cap, hidden).astype(F32) * norm_gain.astype(F32)
    dx = (r * (u - xh * jnp.mean(u * xh, axis=-1, keepdims=True))).astype(BF16)
    grad_table = jax.ops.segment_sum(dx.astype(F32), jnp.where(wanted >= 0, wanted, rows), num_segments=rows)
    return y.reshape(grad_block.shape), grad_table, jnp.sum(dg, axis=0)


def call(kernel, name, out_shape, in_specs, out_specs, scratch_shapes, flops, limit, aliases=None, **params):
    return pl.pallas_call(
        kernel, out_shape=out_shape, in_specs=in_specs, out_specs=out_specs, scratch_shapes=scratch_shapes, name=name,
        input_output_aliases=aliases or {}, cost_estimate=pl.CostEstimate(flops=flops, bytes_accessed=2**24, transcendentals=0),
        compiler_params=pltpu.CompilerParams(vmem_limit_bytes=limit * 2**20, **params))


def device_step(n, token_ids, table_block, norm_gain, grad_block):
    positions = grad_block.shape[0] * grad_block.shape[1]
    rows, hidden = table_block.shape
    ids = token_ids.reshape(n, positions)
    chips = n // CORES
    slots = chips * X_ROWS
    zero_rows = divisor(rows, ZERO_ROWS)
    shape = jax.ShapeDtypeStruct
    gain = norm_gain.reshape(hidden // 128, 128)
    slabs = rows // 8
    xpos, sums, dg, target, over = call(
        functools.partial(exchange_kernel, n, rows), 'exchange',
        (shape((positions, hidden), BF16), shape((slots, hidden), F32), shape((1, hidden), F32), shape((8, slots), I32), shape((1, 1), I32)),
        [anywhere()] * 4, (vmem(),) * 4 + (anywhere(),),
        [pltpu.SMEM((1, 1), I32), pltpu.VMEM((n, positions), I32), pltpu.VMEM((hidden // 128, 128), BF16), pltpu.VMEM((positions, hidden), BF16), pltpu.VMEM((slabs, 8, hidden), BF16), pltpu.VMEM((X_ROWS, 8, hidden), BF16), pltpu.VMEM((8, slots), I32), pltpu.SMEM((8, slots), I32),
         pltpu.VMEM((chips, X_ROWS, hidden), BF16), pltpu.VMEM((n, X_ROWS, hidden), BF16), pltpu.VMEM((chips, DY_ROWS, hidden), BF16),
         pltpu.VMEM((n, DY_ROWS, hidden), BF16), pltpu.VMEM((n, DY_ROWS, slots), BF16), pltpu.VMEM((n, DY_ROWS, slots), BF16),
         pltpu.VMEM((n, DY_ROWS, hidden), BF16), pltpu.VMEM((n, 1, hidden), F32), dma(max(d for d in range(1, 11) if slabs % d == 0)), pltpu.SemaphoreType.DMA, dma(3)]
        + [dma(chips)] * 8 + [dma(n)] * 2, 10**9, 48, collective_id=0, has_side_effects=True)(
            ids, table_block.reshape(slabs, 8, hidden), grad_block.reshape(positions, hidden), gain)
    y, grad_table, dg = call(
        functools.partial(finish_kernel, zero_rows), 'finish',
        (shape((positions, hidden), BF16), shape((rows, hidden), F32), shape((hidden // 128, 128), F32)),
        [anywhere()] + [vmem()] * 4, (anywhere(),) * 3,
        [pltpu.VMEM((zero_rows, hidden), F32), pltpu.SMEM((8, slots), I32), pltpu.VMEM((positions, hidden), BF16), pltpu.VMEM((hidden // 128, 128), F32),
         dma(rows // zero_rows), pltpu.SemaphoreType.DMA, pltpu.SemaphoreType.DMA, dma(2)],
        10**9, 36)(target, xpos, sums, gain, dg)
    result = y.reshape(grad_block.shape), grad_table, dg.reshape(hidden)

    def general(carry):
        return (jnp.zeros((), I32),) + any_path(n, ids, table_block, norm_gain, grad_block)

    return lax.while_loop(lambda carry: carry[0] > 0, general, (over[0, 0],) + result)[1:]


def solution(mesh):
    return jax.shard_map(functools.partial(device_step, mesh.shape['tp']), mesh=mesh, in_specs=(P('dp', None), P('tp', None), P(None), P('dp', 'tp', None)), out_specs=(P('dp', 'tp', None), P(('dp', 'tp'), None), P('dp')), check_vma=False)
```

```python
import functools

import jax
import jax.numpy as jnp
from jax import lax
from jax.experimental import pallas as pl
from jax.experimental.pallas import tpu as pltpu
from jax.sharding import PartitionSpec as P

RMS_EPS = 1e-5
CORES = 2
X_ROWS = 40
DY_ROWS = 56
ZERO_ROWS = 160
MESH = pl.DeviceIdType.MESH
F32 = jnp.float32
BF16 = jnp.bfloat16
I32 = jnp.int32
NT = (((1,), (1,)), ((), ()))
TN = (((0,), (0,)), ((), ()))
LIMIT = 60 * 2**20


def iota(shape, dim):
    return lax.broadcasted_iota(I32, shape, dim)


def divisor(rows, most):
    return max(d for d in range(8, most + 1, 8) if rows % d == 0)


def rms(h):
    return lax.rsqrt(jnp.mean(h * h, axis=-1, keepdims=True) + RMS_EPS)


def column(row):
    size = row.shape[1]
    return jnp.sum(jnp.where(iota((size, size), 0) == iota((size, size), 1), row, 0.0), axis=1, keepdims=True)


def firsts(even, odd):
    size = even.shape[1]
    before = iota((size, size), 0) < iota((size, size), 1)
    even_col, odd_col = column(even), column(odd)
    even_dup = jnp.where((even_col == even) & before, 1.0, 0.0)
    odd_dup = jnp.where((even_col == odd) | ((odd_col == odd) & before), 1.0, 0.0)
    return 1.0 - jnp.max(even_dup, axis=0, keepdims=True), 1.0 - jnp.max(odd_dup, axis=0, keepdims=True)


def one_hots(mask, offset, cap):
    size = mask.shape[1]
    before = (iota((size, size), 0) < iota((size, size), 1)).astype(BF16)
    rank = jnp.dot(mask.astype(BF16), before, preferred_element_type=F32)
    if offset is not None:
        rank = rank + offset
    rank = jnp.where(mask > 0.0, rank, -1.0).astype(I32)
    slots = iota((cap, size), 0)
    return jnp.concatenate([jnp.where(rank[i:i + 1] == slots, 1.0, 0.0) for i in range(mask.shape[0])], axis=0)


def halves(ids):
    code = ids + 1
    return (code >> 8).astype(F32), (code & 255).astype(F32)


def unique_lists(even_mask, odd_mask, even_code, odd_code, cap):
    even_hot = one_hots(even_mask, None, cap)
    odd_hot = one_hots(odd_mask, jnp.sum(even_mask, axis=1, keepdims=True), cap)
    return (lax.dot_general(even_code.astype(BF16), even_hot.astype(BF16), NT, preferred_element_type=F32)
            + lax.dot_general(odd_code.astype(BF16), odd_hot.astype(BF16), NT, preferred_element_type=F32))


def wide(lines):
    lines = lines.astype(F32)
    return jnp.concatenate([lines[i:i + 1] for i in range(lines.shape[0])], axis=1)


def within(ids, low, high):
    return jnp.where((ids >= low) & (ids < high), 1.0, 0.0)


def exchange_kernel(n, rows, ids_hbm, table_hbm, dy_hbm, g_hbm, xpos_ref, sums_ref, dg_ref, target_ref, over_hbm,
                    over_ref, ids_ref, g_ref, dy_own, table, slabs, local, local_smem, x_own, x_in, dy_out, dy_in, picks, spots, dx_all, dg_parts, dg_chips,
                    table_sem, small_sem, own_sem, x_send, x_recv, xf_send, xf_recv, dy_send, dy_recv, dyf_send, dyf_recv, dg_send, dg_recv):
    chips = n // CORES
    me = lax.axis_index('tp')
    dp = lax.axis_index('dp')
    chip = me // CORES
    core = me % CORES
    partner = chip * CORES + 1 - core
    slots, hidden = sums_ref.shape
    barrier = pltpu.get_barrier_semaphore()
    for device in [lax.rem(chip + step, chips) * CORES + core for step in range(1, chips)] + [partner]:
        pl.semaphore_signal(barrier, inc=1, device_id=(dp, device), device_id_type=MESH)
    load_ids = pltpu.make_async_copy(ids_hbm, ids_ref, own_sem.at[0])
    load_dy = pltpu.make_async_copy(dy_hbm, dy_own, own_sem.at[1])
    load_gain = pltpu.make_async_copy(g_hbm, g_ref, own_sem.at[2])
    for copy in (load_ids, load_dy, load_gain):
        copy.start()
    pieces = table_sem.shape[0]
    piece = table_hbm.shape[0] // pieces
    table_copies = [pltpu.make_async_copy(table_hbm.at[pl.ds(i * piece, piece)], table.at[pl.ds(i * piece, piece)], table_sem.at[i]) for i in range(pieces)]
    def remote(src, dst, send_sem, recv_sem, device):
        return pltpu.make_async_remote_copy(src_ref=src, dst_ref=dst, send_sem=send_sem, recv_sem=recv_sem, device_id=(dp, device), device_id_type=MESH)

    sent = []

    def send(*args):
        copy = remote(*args)
        copy.start()
        sent.append(copy)

    def source(step):
        return lax.rem(chip + chips - step, chips)

    def device_at(step):
        return lax.rem(chip + step, chips) * CORES + core

    order = list(range(2, chips - 1)) + [chips - 1, 1]
    low = me * rows

    load_ids.wait()
    my_ids = ids_ref[pl.ds(me, 1)]
    near = [lax.rem(chip + step, chips) for step in range(chips)]
    masks = jnp.concatenate([within(my_ids, c * CORES * rows, (c + 1) * CORES * rows) for c in near], axis=0)
    hots = one_hots(masks, None, DY_ROWS).astype(BF16)
    load_dy.wait()
    load_gain.wait()
    for copy in table_copies:
        copy.start()
    lists = jnp.dot(hots, dy_own[...], preferred_element_type=F32).astype(BF16)
    for step in range(chips):
        dy_out[step] = lists[step * DY_ROWS:(step + 1) * DY_ROWS]
    pl.semaphore_wait(barrier, chips)
    for step in order:
        send(dy_out.at[step], dy_in.at[me], dy_send.at[step], dy_recv.at[step], device_at(step))
    send(dy_out.at[0], dy_in.at[me], dyf_send.at[0], dyf_recv.at[0], partner)
    dy_in[me] = dy_out[0]

    even = jnp.concatenate([ids_ref[pl.ds(c * CORES, 1)] for c in near], axis=0)
    odd = jnp.concatenate([ids_ref[pl.ds(c * CORES + 1, 1)] for c in near], axis=0)
    near_even, near_odd = even, odd
    even_f, odd_f = even.astype(F32), odd.astype(F32)
    flags = [firsts(even_f[d:d + 1], odd_f[d:d + 1]) for d in range(chips)]
    even_first = jnp.concatenate([f[0] for f in flags], axis=0)
    odd_first = jnp.concatenate([f[1] for f in flags], axis=0)
    even_code = jnp.concatenate(halves(even), axis=0)
    odd_code = jnp.concatenate(halves(odd), axis=0)
    product = unique_lists(within(even, low, low + rows) * even_first, within(odd, low, low + rows) * odd_first, even_code, odd_code, X_ROWS)
    row_of, slot_of = iota(product.shape, 0), iota(product.shape, 1)
    own_block = (row_of % chips) == (slot_of // X_ROWS)
    wanted = jnp.sum(jnp.where(own_block, product * jnp.where(row_of < chips, 256.0, 1.0), 0.0), axis=0, keepdims=True) - 1.0
    row_in_block = jnp.clip(wanted.astype(I32) - low, 0, rows - 1)
    local[...] = jnp.broadcast_to(row_in_block >> 3, local.shape)
    to_smem = pltpu.make_async_copy(local, local_smem, small_sem)
    to_smem.start()
    remainder = column((row_in_block & 7).astype(F32)).astype(I32)
    wanted_col = column(wanted)
    earlier = iota((slots, slots), 0) < iota((slots, slots), 1)
    repeated = jnp.max(jnp.where((wanted_col == wanted) & earlier, 1.0, 0.0), axis=0, keepdims=True)
    first_list = jnp.where(repeated > 0.0, -1.0, wanted)
    hot_row, hot_col = iota((X_ROWS, X_ROWS * 8), 0), iota((X_ROWS, X_ROWS * 8), 1)
    for copy in table_copies:
        copy.wait()
    to_smem.wait()
    for step in order + [0]:
        def load(s, _, base=step * X_ROWS):
            for j in range(8):
                k = s * 8 + j
                slabs[k] = table[jnp.clip(local_smem[0, base + k], 0, table.shape[0] - 1)]
            return 0
        lax.fori_loop(0, X_ROWS // 8, load, 0)
        pick = jnp.where(hot_col == hot_row * 8 + remainder[step * X_ROWS:(step + 1) * X_ROWS], 1.0, 0.0).astype(BF16)
        x_own[step] = jnp.dot(pick, slabs[...].reshape(X_ROWS * 8, hidden), preferred_element_type=F32).astype(BF16)
        if step:
            send(x_own.at[step], x_in.at[me], x_send.at[step], x_recv.at[step], device_at(step))
        else:
            send(x_own.at[0], x_in.at[me], xf_send.at[0], xf_recv.at[0], partner)
            x_in[me] = x_own[0]

    key = jnp.where(first_list >= 0.0, first_list, float(n * rows))
    key_col = column(key)
    rank = jnp.sum(jnp.where((key_col < key) | ((key_col == key) & earlier), 1.0, 0.0), axis=0, keepdims=True)
    rank_col = column(rank)
    first_col = column(first_list)
    sorted_list = jnp.sum(jnp.where(rank_col == iota((slots, slots), 1).astype(F32), first_col, 0.0), axis=0, keepdims=True)
    target_ref[...] = jnp.broadcast_to(jnp.where(sorted_list >= 0.0, sorted_list - low.astype(F32), float(n * rows)).astype(I32), target_ref.shape)
    ids = ids_ref[...]
    all_hots = one_hots(within(ids, chip * CORES * rows, (chip + 1) * CORES * rows), None, DY_ROWS)
    for i in range(n):
        code = (ids[i:i + 1] + 2).astype(F32)
        row_ids = jnp.sum(all_hots[i * DY_ROWS:(i + 1) * DY_ROWS] * code, axis=1, keepdims=True) - 2.0
        picks[i] = jnp.where(row_ids == first_list, 1.0, 0.0).astype(BF16)
        spots[i] = jnp.where(row_ids == sorted_list, 1.0, 0.0).astype(BF16)
    gain32 = wide(g_ref[...])
    x_rows = x_own[...].reshape(slots, hidden)

    def dx_of(block):
        h = jnp.dot(picks[block], x_rows, preferred_element_type=F32)
        r = rms(h)
        xh = h * r
        dy = dy_in[block].astype(F32)
        u = dy * gain32
        dx_all[block] = (r * (u - xh * jnp.mean(u * xh, axis=-1, keepdims=True))).astype(BF16)
        return jnp.sum(dy * xh, axis=0, keepdims=True)

    part = dx_of(me)
    for step in order:
        block = source(step) * CORES + core
        remote(dy_in.at[block], dy_in.at[block], dy_send.at[step], dy_recv.at[step], partner).wait_recv()
        send(dy_in.at[block], dy_in.at[block], dyf_send.at[step], dyf_recv.at[step], partner)
        part = part + dx_of(block)
    for step in [0] + order:
        block = source(step) * CORES + 1 - core
        remote(dy_in.at[block], dy_in.at[block], dyf_send.at[step], dyf_recv.at[step], partner).wait_recv()
        part = part + dx_of(block)
    dg_parts[core] = part
    send(dg_parts.at[core], dg_parts.at[core], dg_send.at[0], dg_recv.at[0], partner)
    length = n * DY_ROWS
    sums_ref[...] = lax.dot_general(spots[...].reshape(length, slots), dx_all[...].reshape(length, hidden), TN, preferred_element_type=F32)
    remote(dg_parts.at[1 - core], dg_parts.at[1 - core], dg_send.at[0], dg_recv.at[0], partner).wait_recv()
    dg_chips[chip] = dg_parts[0] + dg_parts[1]
    for step in range(1, chips):
        send(dg_chips.at[chip], dg_chips.at[chip], dg_send.at[step], dg_recv.at[step], device_at(step))

    even, odd = ids_ref[pl.ds(chip * CORES, 1)], ids_ref[pl.ds(chip * CORES + 1, 1)]
    here_even, here_odd = even_first[0:1], odd_first[0:1]
    even_mask = jnp.concatenate([within(even, i * rows, (i + 1) * rows) for i in range(n)], axis=0) * here_even
    odd_mask = jnp.concatenate([within(odd, i * rows, (i + 1) * rows) for i in range(n)], axis=0) * here_odd
    pad = jnp.zeros((6, even.shape[1]), F32)
    product = unique_lists(even_mask, odd_mask, jnp.concatenate(halves(even) + (pad,), axis=0), jnp.concatenate(halves(odd) + (pad,), axis=0), X_ROWS)
    held = product[0:1] * 256.0 + product[1:2] - 1.0
    pick = jnp.where(column(my_ids.astype(F32)) == held, 1.0, 0.0).astype(BF16)
    most = jnp.zeros((1, 1), F32)
    for i in range(n):
        count = within(near_even, i * rows, i * rows + rows) * even_first + within(near_odd, i * rows, i * rows + rows) * odd_first
        most = jnp.maximum(most, jnp.max(jnp.sum(count, axis=1, keepdims=True) * (1.0 / X_ROWS), axis=0, keepdims=True))
    for c in range(chips):
        count = jnp.sum(within(ids, c * CORES * rows, (c + 1) * CORES * rows), axis=1, keepdims=True)
        most = jnp.maximum(most, jnp.max(count * (1.0 / DY_ROWS), axis=0, keepdims=True))
    over_ref[0, 0] = jnp.where(most > 1.0005, 1, 0)[0, 0]
    put_over = pltpu.make_async_copy(over_ref, over_hbm, own_sem.at[0])
    put_over.start()
    for step in order:
        block = source(step) * CORES + core
        remote(x_in.at[block], x_in.at[block], x_send.at[step], x_recv.at[step], partner).wait_recv()
        send(x_in.at[block], x_in.at[block], xf_send.at[step], xf_recv.at[step], partner)
    for step in range(1, chips):
        block = dg_chips.at[source(step)]
        remote(block, block, dg_send.at[step], dg_recv.at[step], partner).wait_recv()
    total = dg_chips[0]
    for c in range(1, chips):
        total = total + dg_chips[c]
    dg_ref[...] = total
    for step in [0] + order:
        block = source(step) * CORES + 1 - core
        remote(x_in.at[block], x_in.at[block], xf_send.at[step], xf_recv.at[step], partner).wait_recv()
    xpos_ref[...] = jnp.dot(pick, x_in[...].reshape(n * X_ROWS, hidden), preferred_element_type=F32).astype(BF16)
    for copy in sent:
        copy.wait_send()
    put_over.wait()


def finish_kernel(zero_rows, target_ref, xpos_ref, sums_ref, g_ref, dg_in, y_hbm, de_ref, dg_hbm, zeros, targets, y_ref, dg_ref, zero_sem, row_sem, small_sem, out_sem):
    blocks = de_ref.shape[0] // zero_rows
    slots = sums_ref.shape[0]
    zeros[...] = jnp.zeros_like(zeros)

    def zero_copy(i):
        return pltpu.make_async_copy(zeros, de_ref.at[pl.ds(pl.multiple_of(i * zero_rows, 8), zero_rows)], zero_sem.at[i])

    for i in range(blocks):
        zero_copy(i).start()
    to_smem = pltpu.make_async_copy(target_ref, targets, small_sem)
    to_smem.start()
    gain = wide(g_ref[...]).astype(BF16)
    h = xpos_ref[...].astype(F32)
    y_ref[...] = (h * rms(h)).astype(BF16) * gain
    for i in range(dg_ref.shape[0]):
        dg_ref[i:i + 1] = dg_in[:, i * 128:(i + 1) * 128]
    outs = [pltpu.make_async_copy(y_ref, y_hbm, out_sem.at[0]), pltpu.make_async_copy(dg_ref, dg_hbm, out_sem.at[1])]
    for copy in outs:
        copy.start()
    to_smem.wait()

    def row_copy(k):
        return pltpu.make_async_copy(sums_ref.at[pl.ds(k, 1)], de_ref.at[pl.ds(targets[0, k], 1)], row_sem)

    def block(i, k):
        zero_copy(i).wait()

        def put(k):
            row_copy(k).start()
            return k + 1
        return lax.while_loop(lambda k: (k < slots) & (targets[0, jnp.minimum(k, slots - 1)] < (i + 1) * zero_rows), put, k)

    count = lax.fori_loop(0, blocks, block, 0)

    def done(k, _):
        row_copy(k).wait()
        return 0

    lax.fori_loop(0, count, done, 0)
    for copy in outs:
        copy.wait()


def vmem():
    return pl.BlockSpec(memory_space=pltpu.VMEM)


def smem():
    return pl.BlockSpec(memory_space=pltpu.SMEM)


def anywhere():
    return pl.BlockSpec(memory_space=pl.ANY)


def dma(*shape):
    return pltpu.SemaphoreType.DMA(shape)


def pair_exchange_kernel(n, x_out, dy_out, x_in, dy_in, dg_ref, dg_parts, x_send, x_recv, dy_send, dy_recv, dg_send, dg_recv):
    me = lax.axis_index('tp')
    dp = lax.axis_index('dp')
    barrier = pltpu.get_barrier_semaphore()
    for step in range(1, n):
        pl.semaphore_signal(barrier, inc=1, device_id=(dp, lax.rem(me + step, n)), device_id_type=MESH)
    pl.semaphore_wait(barrier, n - 1)

    def copies(src, dst, send_sem, recv_sem, step):
        peer = lax.rem(me + step, n)
        return pltpu.make_async_remote_copy(
            src_ref=src.at[peer], dst_ref=dst.at[me], send_sem=send_sem.at[step], recv_sem=recv_sem.at[step],
            device_id=(dp, peer), device_id_type=MESH)

    def arrival(dst, send_sem, recv_sem, step):
        source = lax.rem(me + n - step, n)
        return pltpu.make_async_remote_copy(
            src_ref=dst.at[source], dst_ref=dst.at[source], send_sem=send_sem.at[step], recv_sem=recv_sem.at[step],
            device_id=(dp, source), device_id_type=MESH)

    x_copies = [copies(x_out, x_in, x_send, x_recv, step) for step in range(1, n)]
    for copy in x_copies:
        copy.start()
    dy_copies = [copies(dy_out, dy_in, dy_send, dy_recv, step) for step in range(1, n)]
    for copy in dy_copies:
        copy.start()
    x_in[me] = x_out[me]
    dy_in[me] = dy_out[me]

    def dg_of(block):
        h = x_in[block].astype(F32)
        return jnp.sum(dy_out[block].astype(F32) * (h * rms(h)), axis=0, keepdims=True)

    for step in range(1, n):
        arrival(x_in, x_send, x_recv, step).wait_recv()
    dg_parts[me] = lax.fori_loop(1, n, lambda i, total: total + dg_of(i), dg_of(0))

    def dg_copy(step):
        return pltpu.make_async_remote_copy(
            src_ref=dg_parts.at[me], dst_ref=dg_parts.at[me], send_sem=dg_send.at[step], recv_sem=dg_recv.at[step],
            device_id=(dp, lax.rem(me + step, n)), device_id_type=MESH)

    dg_copies = [dg_copy(step) for step in range(1, n)]
    for copy in dg_copies:
        copy.start()
    for step in range(1, n):
        arrival(dy_in, dy_send, dy_recv, step).wait_recv()
    for step in range(1, n):
        arrival(dg_parts, dg_send, dg_recv, step).wait_recv()
    for i in range(n):
        dg_ref[i:i + 1] = dg_parts[i]
    for copy in x_copies + dy_copies + dg_copies:
        copy.wait_send()


def any_path(n, ids, table_block, norm_gain, grad_block):
    rows, hidden = table_block.shape
    positions = ids.shape[1]
    cap = positions
    me = lax.axis_index('tp')
    before = (iota((positions, positions), 0) < iota((positions, positions), 1)).astype(I32)

    def slots_of(mask):
        return jnp.sum(mask.astype(I32)[:, :, None] * before[None], axis=1)

    local = ids - me * rows
    mine = (local >= 0) & (local < rows)
    slot = slots_of(mine)
    hit = mine[:, None, :] & (slot[:, None, :] == jnp.arange(cap)[None, :, None])
    wanted = jnp.sum(jnp.where(hit, local[:, None, :] + 1, 0), axis=-1).reshape(n * cap) - 1
    x_own = jnp.take(table_block, jnp.maximum(wanted, 0), axis=0)
    my_ids = lax.dynamic_index_in_dim(ids, me, 0, keepdims=True)
    starts = jnp.arange(n, dtype=I32)[:, None] * rows
    theirs = (my_ids >= starts) & (my_ids < starts + rows)
    their_slot = slots_of(theirs)
    hot = theirs[:, None, :] & (their_slot[:, None, :] == jnp.arange(cap)[None, :, None])
    dy_out = jnp.dot(hot.reshape(n * cap, positions).astype(BF16), grad_block.reshape(positions, hidden))
    slot_of = jnp.sum(jnp.where(theirs, jnp.arange(n)[:, None] * cap + their_slot, 0), axis=0)
    x_in, dy_in, dg = pl.pallas_call(
        functools.partial(pair_exchange_kernel, n),
        out_shape=(jax.ShapeDtypeStruct((n, cap, hidden), BF16), jax.ShapeDtypeStruct((n, cap, hidden), BF16), jax.ShapeDtypeStruct((n, hidden), F32)),
        in_specs=[vmem(), vmem()],
        out_specs=(vmem(), vmem(), vmem()),
        scratch_shapes=[pltpu.VMEM((n, 1, hidden), F32)] + [dma(n)] * 6,
        compiler_params=pltpu.CompilerParams(collective_id=1, has_side_effects=True, vmem_limit_bytes=LIMIT),
        name='exchange_pairs',
    )(x_own.reshape(n, cap, hidden), dy_out.reshape(n, cap, hidden))
    h = jnp.take(x_in.reshape(n * cap, hidden), slot_of, axis=0).astype(F32)
    y = (h * rms(h)).astype(BF16) * norm_gain
    h = x_own.astype(F32)
    r = rms(h)
    xh = h * r
    u = dy_in.reshape(n * cap, hidden).astype(F32) * norm_gain.astype(F32)
    dx = (r * (u - xh * jnp.mean(u * xh, axis=-1, keepdims=True))).astype(BF16)
    grad_table = jax.ops.segment_sum(dx.astype(F32), jnp.where(wanted >= 0, wanted, rows), num_segments=rows)
    return y.reshape(grad_block.shape), grad_table, jnp.sum(dg, axis=0)


def call(kernel, name, out_shape, in_specs, out_specs, scratch_shapes, flops, limit, aliases=None, **params):
    return pl.pallas_call(
        kernel, out_shape=out_shape, in_specs=in_specs, out_specs=out_specs, scratch_shapes=scratch_shapes, name=name,
        input_output_aliases=aliases or {}, cost_estimate=pl.CostEstimate(flops=flops, bytes_accessed=2**24, transcendentals=0),
        compiler_params=pltpu.CompilerParams(vmem_limit_bytes=limit * 2**20, **params))


def device_step(n, token_ids, table_block, norm_gain, grad_block):
    positions = grad_block.shape[0] * grad_block.shape[1]
    rows, hidden = table_block.shape
    ids = token_ids.reshape(n, positions)
    chips = n // CORES
    slots = chips * X_ROWS
    zero_rows = divisor(rows, ZERO_ROWS)
    shape = jax.ShapeDtypeStruct
    gain = norm_gain.reshape(hidden // 128, 128)
    slabs = rows // 8
    xpos, sums, dg, target, over = call(
        functools.partial(exchange_kernel, n, rows), 'exchange',
        (shape((positions, hidden), BF16), shape((slots, hidden), F32), shape((1, hidden), F32), shape((8, slots), I32), shape((1, 1), I32)),
        [anywhere()] * 4, (vmem(),) * 4 + (anywhere(),),
        [pltpu.SMEM((1, 1), I32), pltpu.VMEM((n, positions), I32), pltpu.VMEM((hidden // 128, 128), BF16), pltpu.VMEM((positions, hidden), BF16), pltpu.VMEM((slabs, 8, hidden), BF16), pltpu.VMEM((X_ROWS, 8, hidden), BF16), pltpu.VMEM((8, slots), I32), pltpu.SMEM((8, slots), I32),
         pltpu.VMEM((chips, X_ROWS, hidden), BF16), pltpu.VMEM((n, X_ROWS, hidden), BF16), pltpu.VMEM((chips, DY_ROWS, hidden), BF16),
         pltpu.VMEM((n, DY_ROWS, hidden), BF16), pltpu.VMEM((n, DY_ROWS, slots), BF16), pltpu.VMEM((n, DY_ROWS, slots), BF16),
         pltpu.VMEM((n, DY_ROWS, hidden), BF16), pltpu.VMEM((CORES, 1, hidden), F32), pltpu.VMEM((chips, 1, hidden), F32), dma(max(d for d in range(1, 11) if slabs % d == 0)), pltpu.SemaphoreType.DMA, dma(3)]
        + [dma(chips)] * 10, 10**9, 48, collective_id=0, has_side_effects=True)(
            ids, table_block.reshape(slabs, 8, hidden), grad_block.reshape(positions, hidden), gain)
    y, grad_table, dg = call(
        functools.partial(finish_kernel, zero_rows), 'finish',
        (shape((positions, hidden), BF16), shape((rows, hidden), F32), shape((hidden // 128, 128), F32)),
        [anywhere()] + [vmem()] * 4, (anywhere(),) * 3,
        [pltpu.VMEM((zero_rows, hidden), F32), pltpu.SMEM((8, slots), I32), pltpu.VMEM((positions, hidden), BF16), pltpu.VMEM((hidden // 128, 128), F32),
         dma(rows // zero_rows), pltpu.SemaphoreType.DMA, pltpu.SemaphoreType.DMA, dma(2)],
        10**9, 36)(target, xpos, sums, gain, dg)
    result = y.reshape(grad_block.shape), grad_table, dg.reshape(hidden)

    def general(carry):
        return (jnp.zeros((), I32),) + any_path(n, ids, table_block, norm_gain, grad_block)

    return lax.while_loop(lambda carry: carry[0] > 0, general, (over[0, 0],) + result)[1:]


def solution(mesh):
    return jax.shard_map(functools.partial(device_step, mesh.shape['tp']), mesh=mesh, in_specs=(P('dp', None), P('tp', None), P(None), P('dp', 'tp', None)), out_specs=(P('dp', 'tp', None), P(('dp', 'tp'), None), P('dp')), check_vma=False)
```

```python
import functools

import jax
import jax.numpy as jnp
from jax import lax
from jax.experimental import pallas as pl
from jax.experimental.pallas import tpu as pltpu
from jax.sharding import PartitionSpec as P

RMS_EPS = 1e-5
CORES = 2
X_ROWS = 40
DY_ROWS = 56
ZERO_ROWS = 160
MESH = pl.DeviceIdType.MESH
F32 = jnp.float32
BF16 = jnp.bfloat16
I32 = jnp.int32
NT = (((1,), (1,)), ((), ()))
TN = (((0,), (0,)), ((), ()))
LIMIT = 60 * 2**20


def iota(shape, dim):
    return lax.broadcasted_iota(I32, shape, dim)


def divisor(rows, most):
    return max(d for d in range(8, most + 1, 8) if rows % d == 0)


def rms(h):
    return lax.rsqrt(jnp.mean(h * h, axis=-1, keepdims=True) + RMS_EPS)


def column(row):
    size = row.shape[1]
    return jnp.sum(jnp.where(iota((size, size), 0) == iota((size, size), 1), row, 0.0), axis=1, keepdims=True)


def firsts(even, odd):
    size = even.shape[1]
    before = iota((size, size), 0) < iota((size, size), 1)
    even_col, odd_col = column(even), column(odd)
    even_dup = jnp.where((even_col == even) & before, 1.0, 0.0)
    odd_dup = jnp.where((even_col == odd) | ((odd_col == odd) & before), 1.0, 0.0)
    return 1.0 - jnp.max(even_dup, axis=0, keepdims=True), 1.0 - jnp.max(odd_dup, axis=0, keepdims=True)


def one_hots(mask, offset, cap):
    size = mask.shape[1]
    before = (iota((size, size), 0) < iota((size, size), 1)).astype(BF16)
    rank = jnp.dot(mask.astype(BF16), before, preferred_element_type=F32)
    if offset is not None:
        rank = rank + offset
    rank = jnp.where(mask > 0.0, rank, -1.0).astype(I32)
    slots = iota((cap, size), 0)
    return jnp.concatenate([jnp.where(rank[i:i + 1] == slots, 1.0, 0.0) for i in range(mask.shape[0])], axis=0)


def halves(ids):
    code = ids + 1
    return (code >> 8).astype(F32), (code & 255).astype(F32)


def unique_lists(even_mask, odd_mask, even_code, odd_code, cap):
    even_hot = one_hots(even_mask, None, cap)
    odd_hot = one_hots(odd_mask, jnp.sum(even_mask, axis=1, keepdims=True), cap)
    return (lax.dot_general(even_code.astype(BF16), even_hot.astype(BF16), NT, preferred_element_type=F32)
            + lax.dot_general(odd_code.astype(BF16), odd_hot.astype(BF16), NT, preferred_element_type=F32))


def wide(lines):
    lines = lines.astype(F32)
    return jnp.concatenate([lines[i:i + 1] for i in range(lines.shape[0])], axis=1)


def within(ids, low, high):
    return jnp.where((ids >= low) & (ids < high), 1.0, 0.0)


def exchange_kernel(n, rows, ids_hbm, table_hbm, dy_hbm, g_hbm, xpos_ref, sums_ref, dg_ref, target_ref, over_hbm,
                    over_ref, ids_ref, g_ref, dy_own, table, slabs, local, local_smem, x_own, x_in, dy_out, dy_in, picks, spots, dx_all, dg_parts, dg_chips,
                    table_sem, small_sem, own_sem, x_send, x_recv, xf_send, xf_recv, dy_send, dy_recv, dyf_send, dyf_recv, dg_send, dg_recv):
    chips = n // CORES
    me = lax.axis_index('tp')
    dp = lax.axis_index('dp')
    chip = me // CORES
    core = me % CORES
    partner = chip * CORES + 1 - core
    slots, hidden = sums_ref.shape
    barrier = pltpu.get_barrier_semaphore()
    for device in [lax.rem(chip + step, chips) * CORES + core for step in list(range(2, chips - 1)) + [1, chips - 1]] + [partner]:
        pl.semaphore_signal(barrier, inc=1, device_id=(dp, device), device_id_type=MESH)
    load_ids = pltpu.make_async_copy(ids_hbm, ids_ref, own_sem.at[0])
    load_dy = pltpu.make_async_copy(dy_hbm, dy_own, own_sem.at[1])
    load_gain = pltpu.make_async_copy(g_hbm, g_ref, own_sem.at[2])
    for copy in (load_ids, load_dy, load_gain):
        copy.start()
    pieces = table_sem.shape[0]
    piece = table_hbm.shape[0] // pieces
    table_copies = [pltpu.make_async_copy(table_hbm.at[pl.ds(i * piece, piece)], table.at[pl.ds(i * piece, piece)], table_sem.at[i]) for i in range(pieces)]
    def remote(src, dst, send_sem, recv_sem, device):
        return pltpu.make_async_remote_copy(src_ref=src, dst_ref=dst, send_sem=send_sem, recv_sem=recv_sem, device_id=(dp, device), device_id_type=MESH)

    sent = []

    def send(*args):
        copy = remote(*args)
        copy.start()
        sent.append(copy)

    def source(step):
        return lax.rem(chip + chips - step, chips)

    def device_at(step):
        return lax.rem(chip + step, chips) * CORES + core

    order = list(range(2, chips - 1)) + [chips - 1, 1]
    low = me * rows

    load_ids.wait()
    my_ids = ids_ref[pl.ds(me, 1)]
    near = [lax.rem(chip + step, chips) for step in range(chips)]
    masks = jnp.concatenate([within(my_ids, c * CORES * rows, (c + 1) * CORES * rows) for c in near], axis=0)
    hots = one_hots(masks, None, DY_ROWS).astype(BF16)
    load_dy.wait()
    load_gain.wait()
    for copy in table_copies:
        copy.start()
    lists = jnp.dot(hots, dy_own[...], preferred_element_type=F32).astype(BF16)
    for step in range(chips):
        dy_out[step] = lists[step * DY_ROWS:(step + 1) * DY_ROWS]
    pl.semaphore_wait(barrier, chips)
    for step in order:
        send(dy_out.at[step], dy_in.at[me], dy_send.at[step], dy_recv.at[step], device_at(step))
    send(dy_out.at[0], dy_in.at[me], dyf_send.at[0], dyf_recv.at[0], partner)
    dy_in[me] = dy_out[0]

    even = jnp.concatenate([ids_ref[pl.ds(c * CORES, 1)] for c in near], axis=0)
    odd = jnp.concatenate([ids_ref[pl.ds(c * CORES + 1, 1)] for c in near], axis=0)
    near_even, near_odd = even, odd
    even_f, odd_f = even.astype(F32), odd.astype(F32)
    flags = [firsts(even_f[d:d + 1], odd_f[d:d + 1]) for d in range(chips)]
    even_first = jnp.concatenate([f[0] for f in flags], axis=0)
    odd_first = jnp.concatenate([f[1] for f in flags], axis=0)
    even_code = jnp.concatenate(halves(even), axis=0)
    odd_code = jnp.concatenate(halves(odd), axis=0)
    product = unique_lists(within(even, low, low + rows) * even_first, within(odd, low, low + rows) * odd_first, even_code, odd_code, X_ROWS)
    row_of, slot_of = iota(product.shape, 0), iota(product.shape, 1)
    own_block = (row_of % chips) == (slot_of // X_ROWS)
    wanted = jnp.sum(jnp.where(own_block, product * jnp.where(row_of < chips, 256.0, 1.0), 0.0), axis=0, keepdims=True) - 1.0
    row_in_block = jnp.clip(wanted.astype(I32) - low, 0, rows - 1)
    local[...] = jnp.broadcast_to(row_in_block >> 3, local.shape)
    to_smem = pltpu.make_async_copy(local, local_smem, small_sem)
    to_smem.start()
    remainder = column((row_in_block & 7).astype(F32)).astype(I32)
    wanted_col = column(wanted)
    earlier = iota((slots, slots), 0) < iota((slots, slots), 1)
    repeated = jnp.max(jnp.where((wanted_col == wanted) & earlier, 1.0, 0.0), axis=0, keepdims=True)
    first_list = jnp.where(repeated > 0.0, -1.0, wanted)
    hot_row, hot_col = iota((X_ROWS, X_ROWS * 8), 0), iota((X_ROWS, X_ROWS * 8), 1)
    for copy in table_copies:
        copy.wait()
    to_smem.wait()
    for step in order + [0]:
        def load(s, _, base=step * X_ROWS):
            for j in range(8):
                k = s * 8 + j
                slabs[k] = table[jnp.clip(local_smem[0, base + k], 0, table.shape[0] - 1)]
            return 0
        lax.fori_loop(0, X_ROWS // 8, load, 0)
        pick = jnp.where(hot_col == hot_row * 8 + remainder[step * X_ROWS:(step + 1) * X_ROWS], 1.0, 0.0).astype(BF16)
        x_own[step] = jnp.dot(pick, slabs[...].reshape(X_ROWS * 8, hidden), preferred_element_type=F32).astype(BF16)
        if step:
            send(x_own.at[step], x_in.at[me], x_send.at[step], x_recv.at[step], device_at(step))
        else:
            send(x_own.at[0], x_in.at[me], xf_send.at[0], xf_recv.at[0], partner)
            x_in[me] = x_own[0]

    key = jnp.where(first_list >= 0.0, first_list, float(n * rows))
    key_col = column(key)
    rank = jnp.sum(jnp.where((key_col < key) | ((key_col == key) & earlier), 1.0, 0.0), axis=0, keepdims=True)
    rank_col = column(rank)
    first_col = column(first_list)
    sorted_list = jnp.sum(jnp.where(rank_col == iota((slots, slots), 1).astype(F32), first_col, 0.0), axis=0, keepdims=True)
    target_ref[...] = jnp.broadcast_to(jnp.where(sorted_list >= 0.0, sorted_list - low.astype(F32), float(n * rows)).astype(I32), target_ref.shape)
    ids = ids_ref[...]
    all_hots = one_hots(within(ids, chip * CORES * rows, (chip + 1) * CORES * rows), None, DY_ROWS)
    for i in range(n):
        code = (ids[i:i + 1] + 2).astype(F32)
        row_ids = jnp.sum(all_hots[i * DY_ROWS:(i + 1) * DY_ROWS] * code, axis=1, keepdims=True) - 2.0
        picks[i] = jnp.where(row_ids == first_list, 1.0, 0.0).astype(BF16)
        spots[i] = jnp.where(row_ids == sorted_list, 1.0, 0.0).astype(BF16)
    gain32 = wide(g_ref[...])
    x_rows = x_own[...].reshape(slots, hidden)

    def dx_of(block):
        h = jnp.dot(picks[block], x_rows, preferred_element_type=F32)
        r = rms(h)
        xh = h * r
        dy = dy_in[block].astype(F32)
        u = dy * gain32
        dx_all[block] = (r * (u - xh * jnp.mean(u * xh, axis=-1, keepdims=True))).astype(BF16)
        return jnp.sum(dy * xh, axis=0, keepdims=True)

    part = dx_of(me)
    for step in order:
        block = source(step) * CORES + core
        remote(dy_in.at[block], dy_in.at[block], dy_send.at[step], dy_recv.at[step], partner).wait_recv()
        send(dy_in.at[block], dy_in.at[block], dyf_send.at[step], dyf_recv.at[step], partner)
        part = part + dx_of(block)
    for step in [0] + order:
        block = source(step) * CORES + 1 - core
        remote(dy_in.at[block], dy_in.at[block], dyf_send.at[step], dyf_recv.at[step], partner).wait_recv()
        part = part + dx_of(block)
    dg_parts[core] = part
    send(dg_parts.at[core], dg_parts.at[core], dg_send.at[0], dg_recv.at[0], partner)
    length = n * DY_ROWS
    sums_ref[...] = lax.dot_general(spots[...].reshape(length, slots), dx_all[...].reshape(length, hidden), TN, preferred_element_type=F32)
    remote(dg_parts.at[1 - core], dg_parts.at[1 - core], dg_send.at[0], dg_recv.at[0], partner).wait_recv()
    dg_chips[chip] = dg_parts[0] + dg_parts[1]
    for step in range(1, chips):
        send(dg_chips.at[chip], dg_chips.at[chip], dg_send.at[step], dg_recv.at[step], device_at(step))

    even, odd = ids_ref[pl.ds(chip * CORES, 1)], ids_ref[pl.ds(chip * CORES + 1, 1)]
    here_even, here_odd = even_first[0:1], odd_first[0:1]
    even_mask = jnp.concatenate([within(even, i * rows, (i + 1) * rows) for i in range(n)], axis=0) * here_even
    odd_mask = jnp.concatenate([within(odd, i * rows, (i + 1) * rows) for i in range(n)], axis=0) * here_odd
    pad = jnp.zeros((6, even.shape[1]), F32)
    product = unique_lists(even_mask, odd_mask, jnp.concatenate(halves(even) + (pad,), axis=0), jnp.concatenate(halves(odd) + (pad,), axis=0), X_ROWS)
    held = product[0:1] * 256.0 + product[1:2] - 1.0
    pick = jnp.where(column(my_ids.astype(F32)) == held, 1.0, 0.0).astype(BF16)
    most = jnp.zeros((1, 1), F32)
    for i in range(n):
        count = within(near_even, i * rows, i * rows + rows) * even_first + within(near_odd, i * rows, i * rows + rows) * odd_first
        most = jnp.maximum(most, jnp.max(jnp.sum(count, axis=1, keepdims=True) * (1.0 / X_ROWS), axis=0, keepdims=True))
    for c in range(chips):
        count = jnp.sum(within(ids, c * CORES * rows, (c + 1) * CORES * rows), axis=1, keepdims=True)
        most = jnp.maximum(most, jnp.max(count * (1.0 / DY_ROWS), axis=0, keepdims=True))
    over_ref[0, 0] = jnp.where(most > 1.0005, 1, 0)[0, 0]
    put_over = pltpu.make_async_copy(over_ref, over_hbm, own_sem.at[0])
    put_over.start()
    for step in order:
        block = source(step) * CORES + core
        remote(x_in.at[block], x_in.at[block], x_send.at[step], x_recv.at[step], partner).wait_recv()
        send(x_in.at[block], x_in.at[block], xf_send.at[step], xf_recv.at[step], partner)
    for step in range(1, chips):
        block = dg_chips.at[source(step)]
        remote(block, block, dg_send.at[step], dg_recv.at[step], partner).wait_recv()
    total = dg_chips[0]
    for c in range(1, chips):
        total = total + dg_chips[c]
    dg_ref[...] = total
    for step in [0] + order:
        block = source(step) * CORES + 1 - core
        remote(x_in.at[block], x_in.at[block], xf_send.at[step], xf_recv.at[step], partner).wait_recv()
    xpos_ref[...] = jnp.dot(pick, x_in[...].reshape(n * X_ROWS, hidden), preferred_element_type=F32).astype(BF16)
    for copy in sent:
        copy.wait_send()
    put_over.wait()


def finish_kernel(zero_rows, target_ref, xpos_ref, sums_ref, g_ref, dg_in, y_hbm, de_ref, dg_hbm, zeros, targets, y_ref, dg_ref, zero_sem, row_sem, small_sem, out_sem):
    blocks = de_ref.shape[0] // zero_rows
    slots = sums_ref.shape[0]
    to_smem = pltpu.make_async_copy(target_ref, targets, small_sem)
    to_smem.start()
    zeros[...] = jnp.zeros_like(zeros)

    def zero_copy(i):
        return pltpu.make_async_copy(zeros, de_ref.at[pl.ds(pl.multiple_of(i * zero_rows, 8), zero_rows)], zero_sem.at[i])

    for i in range(blocks):
        zero_copy(i).start()
    gain = wide(g_ref[...]).astype(BF16)
    h = xpos_ref[...].astype(F32)
    y_ref[...] = (h * rms(h)).astype(BF16) * gain
    for i in range(dg_ref.shape[0]):
        dg_ref[i:i + 1] = dg_in[:, i * 128:(i + 1) * 128]
    outs = [pltpu.make_async_copy(y_ref, y_hbm, out_sem.at[0]), pltpu.make_async_copy(dg_ref, dg_hbm, out_sem.at[1])]
    for copy in outs:
        copy.start()
    to_smem.wait()

    def row_copy(k):
        return pltpu.make_async_copy(sums_ref.at[pl.ds(k, 1)], de_ref.at[pl.ds(targets[0, k], 1)], row_sem)

    def block(i, k):
        zero_copy(i).wait()

        def put(k):
            row_copy(k).start()
            return k + 1
        return lax.while_loop(lambda k: (k < slots) & (targets[0, jnp.minimum(k, slots - 1)] < (i + 1) * zero_rows), put, k)

    count = lax.fori_loop(0, blocks, block, 0)

    def done(k, _):
        row_copy(k).wait()
        return 0

    lax.fori_loop(0, count, done, 0)
    for copy in outs:
        copy.wait()


def vmem():
    return pl.BlockSpec(memory_space=pltpu.VMEM)


def smem():
    return pl.BlockSpec(memory_space=pltpu.SMEM)


def anywhere():
    return pl.BlockSpec(memory_space=pl.ANY)


def dma(*shape):
    return pltpu.SemaphoreType.DMA(shape)


def pair_exchange_kernel(n, x_out, dy_out, x_in, dy_in, dg_ref, dg_parts, x_send, x_recv, dy_send, dy_recv, dg_send, dg_recv):
    me = lax.axis_index('tp')
    dp = lax.axis_index('dp')
    barrier = pltpu.get_barrier_semaphore()
    for step in range(1, n):
        pl.semaphore_signal(barrier, inc=1, device_id=(dp, lax.rem(me + step, n)), device_id_type=MESH)
    pl.semaphore_wait(barrier, n - 1)

    def copies(src, dst, send_sem, recv_sem, step):
        peer = lax.rem(me + step, n)
        return pltpu.make_async_remote_copy(
            src_ref=src.at[peer], dst_ref=dst.at[me], send_sem=send_sem.at[step], recv_sem=recv_sem.at[step],
            device_id=(dp, peer), device_id_type=MESH)

    def arrival(dst, send_sem, recv_sem, step):
        source = lax.rem(me + n - step, n)
        return pltpu.make_async_remote_copy(
            src_ref=dst.at[source], dst_ref=dst.at[source], send_sem=send_sem.at[step], recv_sem=recv_sem.at[step],
            device_id=(dp, source), device_id_type=MESH)

    x_copies = [copies(x_out, x_in, x_send, x_recv, step) for step in range(1, n)]
    for copy in x_copies:
        copy.start()
    dy_copies = [copies(dy_out, dy_in, dy_send, dy_recv, step) for step in range(1, n)]
    for copy in dy_copies:
        copy.start()
    x_in[me] = x_out[me]
    dy_in[me] = dy_out[me]

    def dg_of(block):
        h = x_in[block].astype(F32)
        return jnp.sum(dy_out[block].astype(F32) * (h * rms(h)), axis=0, keepdims=True)

    for step in range(1, n):
        arrival(x_in, x_send, x_recv, step).wait_recv()
    dg_parts[me] = lax.fori_loop(1, n, lambda i, total: total + dg_of(i), dg_of(0))

    def dg_copy(step):
        return pltpu.make_async_remote_copy(
            src_ref=dg_parts.at[me], dst_ref=dg_parts.at[me], send_sem=dg_send.at[step], recv_sem=dg_recv.at[step],
            device_id=(dp, lax.rem(me + step, n)), device_id_type=MESH)

    dg_copies = [dg_copy(step) for step in range(1, n)]
    for copy in dg_copies:
        copy.start()
    for step in range(1, n):
        arrival(dy_in, dy_send, dy_recv, step).wait_recv()
    for step in range(1, n):
        arrival(dg_parts, dg_send, dg_recv, step).wait_recv()
    for i in range(n):
        dg_ref[i:i + 1] = dg_parts[i]
    for copy in x_copies + dy_copies + dg_copies:
        copy.wait_send()


def any_path(n, ids, table_block, norm_gain, grad_block):
    rows, hidden = table_block.shape
    positions = ids.shape[1]
    cap = positions
    me = lax.axis_index('tp')
    before = (iota((positions, positions), 0) < iota((positions, positions), 1)).astype(I32)

    def slots_of(mask):
        return jnp.sum(mask.astype(I32)[:, :, None] * before[None], axis=1)

    local = ids - me * rows
    mine = (local >= 0) & (local < rows)
    slot = slots_of(mine)
    hit = mine[:, None, :] & (slot[:, None, :] == jnp.arange(cap)[None, :, None])
    wanted = jnp.sum(jnp.where(hit, local[:, None, :] + 1, 0), axis=-1).reshape(n * cap) - 1
    x_own = jnp.take(table_block, jnp.maximum(wanted, 0), axis=0)
    my_ids = lax.dynamic_index_in_dim(ids, me, 0, keepdims=True)
    starts = jnp.arange(n, dtype=I32)[:, None] * rows
    theirs = (my_ids >= starts) & (my_ids < starts + rows)
    their_slot = slots_of(theirs)
    hot = theirs[:, None, :] & (their_slot[:, None, :] == jnp.arange(cap)[None, :, None])
    dy_out = jnp.dot(hot.reshape(n * cap, positions).astype(BF16), grad_block.reshape(positions, hidden))
    slot_of = jnp.sum(jnp.where(theirs, jnp.arange(n)[:, None] * cap + their_slot, 0), axis=0)
    x_in, dy_in, dg = pl.pallas_call(
        functools.partial(pair_exchange_kernel, n),
        out_shape=(jax.ShapeDtypeStruct((n, cap, hidden), BF16), jax.ShapeDtypeStruct((n, cap, hidden), BF16), jax.ShapeDtypeStruct((n, hidden), F32)),
        in_specs=[vmem(), vmem()],
        out_specs=(vmem(), vmem(), vmem()),
        scratch_shapes=[pltpu.VMEM((n, 1, hidden), F32)] + [dma(n)] * 6,
        compiler_params=pltpu.CompilerParams(collective_id=1, has_side_effects=True, vmem_limit_bytes=LIMIT),
        name='exchange_pairs',
    )(x_own.reshape(n, cap, hidden), dy_out.reshape(n, cap, hidden))
    h = jnp.take(x_in.reshape(n * cap, hidden), slot_of, axis=0).astype(F32)
    y = (h * rms(h)).astype(BF16) * norm_gain
    h = x_own.astype(F32)
    r = rms(h)
    xh = h * r
    u = dy_in.reshape(n * cap, hidden).astype(F32) * norm_gain.astype(F32)
    dx = (r * (u - xh * jnp.mean(u * xh, axis=-1, keepdims=True))).astype(BF16)
    grad_table = jax.ops.segment_sum(dx.astype(F32), jnp.where(wanted >= 0, wanted, rows), num_segments=rows)
    return y.reshape(grad_block.shape), grad_table, jnp.sum(dg, axis=0)


def call(kernel, name, out_shape, in_specs, out_specs, scratch_shapes, flops, limit, aliases=None, **params):
    return pl.pallas_call(
        kernel, out_shape=out_shape, in_specs=in_specs, out_specs=out_specs, scratch_shapes=scratch_shapes, name=name,
        input_output_aliases=aliases or {}, cost_estimate=pl.CostEstimate(flops=flops, bytes_accessed=2**24, transcendentals=0),
        compiler_params=pltpu.CompilerParams(vmem_limit_bytes=limit * 2**20, **params))


def device_step(n, token_ids, table_block, norm_gain, grad_block):
    positions = grad_block.shape[0] * grad_block.shape[1]
    rows, hidden = table_block.shape
    ids = token_ids.reshape(n, positions)
    chips = n // CORES
    slots = chips * X_ROWS
    zero_rows = divisor(rows, ZERO_ROWS)
    shape = jax.ShapeDtypeStruct
    gain = norm_gain.reshape(hidden // 128, 128)
    slabs = rows // 8
    xpos, sums, dg, target, over = call(
        functools.partial(exchange_kernel, n, rows), 'exchange',
        (shape((positions, hidden), BF16), shape((slots, hidden), F32), shape((1, hidden), F32), shape((8, slots), I32), shape((1, 1), I32)),
        [anywhere()] * 4, (vmem(),) * 4 + (anywhere(),),
        [pltpu.SMEM((1, 1), I32), pltpu.VMEM((n, positions), I32), pltpu.VMEM((hidden // 128, 128), BF16), pltpu.VMEM((positions, hidden), BF16), pltpu.VMEM((slabs, 8, hidden), BF16), pltpu.VMEM((X_ROWS, 8, hidden), BF16), pltpu.VMEM((8, slots), I32), pltpu.SMEM((8, slots), I32),
         pltpu.VMEM((chips, X_ROWS, hidden), BF16), pltpu.VMEM((n, X_ROWS, hidden), BF16), pltpu.VMEM((chips, DY_ROWS, hidden), BF16),
         pltpu.VMEM((n, DY_ROWS, hidden), BF16), pltpu.VMEM((n, DY_ROWS, slots), BF16), pltpu.VMEM((n, DY_ROWS, slots), BF16),
         pltpu.VMEM((n, DY_ROWS, hidden), BF16), pltpu.VMEM((CORES, 1, hidden), F32), pltpu.VMEM((chips, 1, hidden), F32), dma(max(d for d in range(1, 11) if slabs % d == 0)), pltpu.SemaphoreType.DMA, dma(3)]
        + [dma(chips)] * 10, 10**9, 48, collective_id=0, has_side_effects=True)(
            ids, table_block.reshape(slabs, 8, hidden), grad_block.reshape(positions, hidden), gain)
    y, grad_table, dg = call(
        functools.partial(finish_kernel, zero_rows), 'finish',
        (shape((positions, hidden), BF16), shape((rows, hidden), F32), shape((hidden // 128, 128), F32)),
        [anywhere()] + [vmem()] * 4, (anywhere(),) * 3,
        [pltpu.VMEM((zero_rows, hidden), F32), pltpu.SMEM((8, slots), I32), pltpu.VMEM((positions, hidden), BF16), pltpu.VMEM((hidden // 128, 128), F32),
         dma(rows // zero_rows), pltpu.SemaphoreType.DMA, pltpu.SemaphoreType.DMA, dma(2)],
        10**9, 36)(target, xpos, sums, gain, dg)
    result = y.reshape(grad_block.shape), grad_table, dg.reshape(hidden)

    def general(carry):
        return (jnp.zeros((), I32),) + any_path(n, ids, table_block, norm_gain, grad_block)

    return lax.while_loop(lambda carry: carry[0] > 0, general, (over[0, 0],) + result)[1:]


def solution(mesh):
    return jax.shard_map(functools.partial(device_step, mesh.shape['tp']), mesh=mesh, in_specs=(P('dp', None), P('tp', None), P(None), P('dp', 'tp', None)), out_specs=(P('dp', 'tp', None), P(('dp', 'tp'), None), P('dp')), check_vma=False)
```
